128 devices in a mesh: ep: 32 (over y, x, core), dp: 4 (over z).
Axes of the slice: x: 4, y: 4, z: 4, core: 2. Of those that a mesh axis runs over, the one named last changes fastest.
Arguments:
- resid: bfloat16 [2048, 4096], P(('ep', 'dp')), may hold values from -6 to 6
- queries: bfloat16 [2048, 8192], P(('ep', 'dp')), may hold values from -4.5 to 4.5
- new_keys: bfloat16 [2048, 512], P(('ep', 'dp')), may hold values from -4.5 to 4.5
- new_values: bfloat16 [2048, 512], P(('ep', 'dp')), may hold values from -6 to 6
- cache_keys: bfloat16 [2048, 128, 512], P(('ep', 'dp')), may hold values from -4.5 to 4.5
- cache_values: bfloat16 [2048, 128, 512], P(('ep', 'dp')), may hold values from -6 to 6
- cache_len: int32 [2048], P(('ep', 'dp')), may hold values from 1 to 128
- out_proj: bfloat16 [8192, 4096], P('ep'), may hold values from -0.0625 to 0.0625
- norm_gain: float32 [4096], replicated, may hold values from 0.1 to 1.9
- router: bfloat16 [4096, 64], replicated, may hold values from -4 to 4
- expert_ids: int32 [2048, 8], P(('ep', 'dp')), may hold values from 0 to 63, all different within a row; in each aligned block of 16 rows (0 to 15, 16 to 31, ...) at most 4 rows name the same one
- gate_slab: bfloat16 [128, 4096, 384], P(('ep', 'dp')), may hold values from -0.09375 to 0.09375
- up_slab: bfloat16 [128, 4096, 384], P(('ep', 'dp')), may hold values from -0.09375 to 0.09375
- down_slab: bfloat16 [128, 384, 4096], P(('ep', 'dp')), may hold values from -0.21875 to 0.21875
Outputs:
- mixed: float32 [2048, 4096], P(('ep', 'dp'))
The draws below stay inside these ranges and needn't reach their ends.
Inputs may be any that keep to these rules, and one draw needn't show every extreme that they name: `expert_ids`: each row names 8 different experts; among the rows of one device no expert is named by more than 4 rows.
All inputs are finite; a program needn't handle non-finite values.
Results may differ from the reference program's by a relative error of at most 0.009.
Values may be sent and summed in bfloat16 or wider, within the bound.
No kernel may reach another device: no remote copies, remote signals or barrier semaphores. Data moves between devices by JAX's collectives and lax.ppermute only.
A program may use at most 128 MiB of HBM per device.

```python
import math
import jax
import jax.numpy as jnp
import numpy as np
from jax import lax

D = 4096
H = 64
KVH = 4
HD = 128
TOP = 8
FF = 768
TOK_DEV = 16
CACHE = 128
EXPERTS = 64
HF = 384
CAP = 4
TOKENS = 2048
N_EP = 32
DEVICES = 128


edge_value = 4.5


def draw_queries(key, part):
    sampled = jnp.clip(jax.random.normal(jax.random.fold_in(key, 1), (TOKENS, H * HD), jnp.float32), -edge_value, edge_value)
    return sampled.astype(jnp.bfloat16)


def draw_cache_keys(key, part):
    sampled = jnp.clip(jax.random.normal(jax.random.fold_in(key, 2), (TOKENS, CACHE, KVH * HD), jnp.float32), -edge_value, edge_value)
    return sampled.astype(jnp.bfloat16)


def draw_router(key, part):
    sampled = jnp.clip(jax.random.normal(jax.random.fold_in(key, 3), (D, EXPERTS), jnp.float32), -4.0, 4.0) / math.sqrt(D)
    return sampled.astype(jnp.bfloat16)


def with_ends(entries, own_key, low, high):
    place = [jax.random.randint(jax.random.fold_in(own_key, axis), (), 0, length) for axis, length in enumerate(entries.shape)]
    main_axis = entries.shape.index(max(entries.shape))
    neighbour = place[:main_axis] + [(place[main_axis] + 1) % entries.shape[main_axis]] + place[main_axis + 1:]
    return entries.at[tuple(place)].set(low).at[tuple(neighbour)].set(high)


def shard_levels(rng, shape, split, least, high):
    loudness, own = 1.0, jax.random.fold_in(rng, 6)
    for axis_at, parts in split:
        steps = jnp.exp(jax.random.uniform(jax.random.fold_in(own, axis_at), (parts,), jnp.float32, least / len(split), high / len(split)))
        loudness = loudness * jnp.repeat(steps, shape[axis_at] // parts).reshape([-1 if axis == axis_at else 1 for axis in range(len(shape))])
    return loudness


def assign_block(rng, own, number, rows, number_of, top, reach, lean):
    order = jax.random.permutation(rng, number_of)
    heavy_load, ordinary = portions_of(number_of, rows * top, reach, lean, True), portions_of(number_of, rows * top, reach, lean, False)
    places = jnp.arange(number_of)

    def named(sizes, offset_by):
        used = int((sizes > 0).sum())
        fixed = max(1, used // 4)
        passed = fixed + (places - fixed + offset_by * (used - fixed)) % max(1, number_of - fixed)
        return jnp.zeros((number_of,), jnp.int32).at[order[jnp.where(places < fixed, places, passed)]].set(jnp.asarray(sizes, jnp.int32))

    sizes = jnp.where(number % 4 == 0, named(heavy_load, number // 4), named(ordinary, number - number // 4 - 1))
    mixed = jax.random.permutation(jax.random.fold_in(own, 3), number_of)
    donor, sink = mixed[0:number_of // 2 * 2:2], mixed[1:number_of // 2 * 2:2]
    margin = jnp.minimum(sizes[donor] - 1, reach - sizes[sink]) // 2
    margin = jnp.where((donor == order[0]) | (sink == order[0]) | (sizes[sink] == 0), 0, jnp.maximum(margin, 0))
    passed = jax.random.randint(jax.random.fold_in(own, 4), (number_of // 2,), 0, 1 << 20) % (margin + 1)
    sizes = sizes.at[donor].add(-passed).at[sink].add(passed)
    labels = jnp.searchsorted(jnp.cumsum(sizes), jnp.arange(rows * top), side="right").astype(jnp.int32)
    listing = labels.reshape(top, rows).T
    listing = listing[jax.random.permutation(jax.random.fold_in(own, 1), rows)]
    offset_by = jax.random.randint(jax.random.fold_in(own, 2), (rows, 1), 0, top)
    return jnp.take_along_axis(listing, (jnp.arange(top)[None, :] + offset_by) % top, axis=1)


def portions_of(count, total, limit, skew, full):
    portions = [(1 << 20) // math.isqrt(rank ** skew) + 1 for rank in range(1, count + 1)]
    largest = limit if full else min(limit, max(-(-total // count), total * portions[0] // sum(portions)))
    least = 1 if total - largest >= count - 1 else 0
    given, spare = [largest] + [least] * (count - 1), total - largest - least * (count - 1)
    while spare > 0:
        movable = [i for i in range(1, count) if given[i] < largest] or [i for i in range(1, count) if given[i] < limit]
        mass, left = sum([portions[i] for i in movable]), spare
        for i in movable:
            addition = min(limit - given[i], max(1, left * portions[i] // mass), spare)
            given[i] = given[i] + addition
            spare = spare - addition
    return np.array(given)


def scatter_about(key, dims, width, reach, cuts=(), held_as=jnp.bfloat16):
    values = width * jax.random.normal(key, dims, jnp.float32)
    if cuts:
        values = values * shard_levels(key, dims, cuts, -0.22, 0.18)
    return jnp.clip(values, -reach, reach).astype(held_as)


def setup_inputs(seed: int = 0) -> dict:
    seeds = jax.random.split(jax.random.key(seed), 15)
    resid = scatter_about(seeds[0], (TOKENS, D), 1.0, 6.0, ((0, 128),))
    queries = draw_queries(jax.random.fold_in(seeds[14], 71), 0)
    new_keys = scatter_about(seeds[2], (TOKENS, KVH * HD), 1.0, 4.5, ((0, 128),))
    new_values = scatter_about(seeds[3], (TOKENS, KVH * HD), 1.0, 6.0, ((0, 128),))
    cache_keys = draw_cache_keys(jax.random.fold_in(seeds[14], 71), 0)
    cache_values = scatter_about(seeds[5], (TOKENS, CACHE, KVH * HD), 1.0, 6.0, ((0, 128),))
    cache_len = with_ends(jax.random.randint(seeds[6], (TOKENS,), 1, CACHE + 1), jax.random.fold_in(seeds[6], 1), 1, CACHE).astype(jnp.int32)
    out_proj = scatter_about(seeds[7], (H * HD, D), (H * HD) ** -0.5, 0.0625, ((0, 32),))
    norm_gain = jnp.clip(1.0 + 0.18 * jax.random.normal(seeds[8], (D,), jnp.float32), 0.1, 1.9)
    router = draw_router(jax.random.fold_in(seeds[14], 71), 0)
    expert_ids_keys = jax.random.split(jax.random.fold_in(seeds[10], 1), TOKENS // TOK_DEV)
    expert_ids_turns = jax.random.permutation(jax.random.fold_in(seeds[10], 3), TOKENS // TOK_DEV)
    expert_ids = jax.vmap(lambda own, number: assign_block(jax.random.fold_in(seeds[10], 2), own, number, TOK_DEV, EXPERTS, TOP, CAP, 2))(expert_ids_keys, expert_ids_turns).reshape((TOKENS, TOP))
    gate_slab = scatter_about(seeds[11], (DEVICES, D, HF), D ** -0.5, 0.09375, ((0, 128),))
    up_slab = scatter_about(seeds[12], (DEVICES, D, HF), D ** -0.5, 0.09375, ((0, 128),))
    down_slab = scatter_about(seeds[13], (DEVICES, HF, D), FF ** -0.5, 0.21875, ((0, 128),))
    return {"resid": resid, "queries": queries, "new_keys": new_keys, "new_values": new_values, "cache_keys": cache_keys, "cache_values": cache_values, "cache_len": cache_len, "out_proj": out_proj, "norm_gain": norm_gain, "router": router, "expert_ids": expert_ids, "gate_slab": gate_slab, "up_slab": up_slab, "down_slab": down_slab}


def attend_block(query_rows, key_new, value_new, key_cache, value_cache, lengths):
    local_rows = query_rows.shape[0]
    cache_span = key_cache.shape[1]
    group_size = H // KVH
    query_heads = query_rows.astype(jnp.float32).reshape(local_rows, KVH, group_size, HD)
    past_keys = key_cache.astype(jnp.float32).reshape(local_rows, cache_span, KVH, HD)
    past_values = value_cache.astype(jnp.float32).reshape(local_rows, cache_span, KVH, HD)
    score_scale = 1.0 / math.sqrt(HD)
    past_scores = jnp.einsum('tgqd,tcgd->tgqc', query_heads, past_keys) * score_scale
    own_scores = jnp.einsum('tgqd,tgd->tgq', query_heads, key_new.astype(jnp.float32).reshape(local_rows, KVH, HD)) * score_scale
    is_valid = lax.broadcasted_iota(jnp.int32, (local_rows, cache_span), 1) < lengths[:, None]
    past_scores = jnp.where(is_valid[:, None, None, :], past_scores, -1e+30)
    peak_score = jnp.maximum(lax.optimization_barrier(jnp.max(past_scores, axis=3)), own_scores)
    past_exp = jnp.exp(past_scores - peak_score[..., None])
    own_exp = jnp.exp(own_scores - peak_score)
    denom_sum = lax.optimization_barrier(jnp.sum(past_exp, axis=3)) + own_exp
    past_weights = lax.optimization_barrier((past_exp / denom_sum[..., None]).astype(jnp.bfloat16))
    own_weights = lax.optimization_barrier((own_exp / denom_sum).astype(jnp.bfloat16))
    blended = jnp.einsum('tgqc,tcgd->tgqd', past_weights.astype(jnp.float32), past_values)
    blended = blended + own_weights.astype(jnp.float32)[..., None] * value_new.astype(jnp.float32).reshape(local_rows, KVH, 1, HD)
    return blended.reshape(local_rows, H * HD).astype(jnp.bfloat16)

def attend_packed(packed):
    return attend_block(*packed)

def blocked(array):
    return array.reshape((DEVICES, TOK_DEV) + array.shape[1:])

def reference(resid, queries, new_keys, new_values, cache_keys, cache_values, cache_len, out_proj, norm_gain, router, expert_ids, gate_slab, up_slab, down_slab):
    packed = (blocked(queries), blocked(new_keys), blocked(new_values), blocked(cache_keys), blocked(cache_values), blocked(cache_len))
    attended = lax.map(attend_packed, packed).reshape(TOKENS, H * HD)
    column_width = H * HD // N_EP
    attn_out = jnp.zeros((TOKENS, D), jnp.float32)
    for shard_index in range(N_EP):
        row_start = shard_index * column_width
        product = jnp.dot(attended[:, row_start:row_start + column_width], out_proj[row_start:row_start + column_width], preferred_element_type=jnp.float32)
        rounded = lax.optimization_barrier(product.astype(jnp.bfloat16))
        attn_out = attn_out + rounded.astype(jnp.float32)
    hidden = resid.astype(jnp.float32) + attn_out
    meansq = lax.optimization_barrier(jnp.mean(hidden * hidden, axis=1, keepdims=True))
    normed = (hidden * lax.rsqrt(jnp.maximum(meansq, 0.25)) * norm_gain).astype(jnp.bfloat16)
    logits = jnp.dot(normed, router, preferred_element_type=jnp.float32)
    chosen = jnp.take_along_axis(logits, expert_ids.astype(jnp.int32), axis=1)
    peak_logit = lax.optimization_barrier(jnp.max(chosen, axis=1, keepdims=True))
    exp_logit = jnp.exp(chosen - peak_logit)
    gate_probs = lax.optimization_barrier((exp_logit / lax.optimization_barrier(jnp.sum(exp_logit, axis=1, keepdims=True))).astype(jnp.bfloat16))
    flat_ids = expert_ids.reshape(-1).astype(jnp.int32)
    token_of = (jnp.arange(TOKENS * TOP, dtype=jnp.int32) // TOP).astype(jnp.int32)
    onehot = (flat_ids[:, None] == jnp.arange(EXPERTS, dtype=jnp.int32)[None, :]).astype(jnp.int32)
    earlier = jnp.cumsum(onehot, axis=0).astype(jnp.int32) - onehot
    ranking = lax.optimization_barrier(jnp.sum(earlier * onehot, axis=1)).astype(jnp.int32)
    row_depth = DEVICES * CAP
    row_table = jnp.zeros((EXPERTS, row_depth), jnp.int32).at[flat_ids, ranking].set(token_of)

    def run_expert(expert):
        rows_in = jnp.take(normed, row_table[expert], axis=0)
        gate_full = jnp.concatenate((gate_slab[2 * expert], gate_slab[2 * expert + 1]), axis=1)
        up_full = jnp.concatenate((up_slab[2 * expert], up_slab[2 * expert + 1]), axis=1)
        down_full = jnp.concatenate((down_slab[2 * expert], down_slab[2 * expert + 1]), axis=0)
        gate_val = jnp.dot(rows_in, gate_full, preferred_element_type=jnp.float32)
        up_val = jnp.dot(rows_in, up_full, preferred_element_type=jnp.float32)
        activated = (jax.nn.silu(gate_val) * up_val).astype(jnp.bfloat16)
        return jnp.dot(activated, down_full, preferred_element_type=jnp.float32).astype(jnp.bfloat16)
    produced = lax.map(run_expert, jnp.arange(EXPERTS, dtype=jnp.int32))
    picked = produced[flat_ids, ranking].reshape(TOKENS, TOP, D)
    expert_mix = jnp.einsum('tk,tkd->td', gate_probs.astype(jnp.float32), picked.astype(jnp.float32))
    return hidden + expert_mix
```

```python
import math

import jax
import jax.numpy as jnp
from jax import lax
from jax.sharding import Mesh
from jax.sharding import PartitionSpec as P

D = 4096
H = 64
KVH = 4
HD = 128
TOP = 8
CAP = 4


EP = ("chip", "core")
ALL = ("chip", "core", "dp")


def flipped(value, axis, mask):
    pairs = [(source, source ^ mask) for source in range(lax.axis_size(axis))]
    return lax.ppermute(value, axis, pairs)


def attend(queries, new_keys, new_values, cache_keys, cache_values, cache_len):
    local_rows = queries.shape[0]
    cache_span = cache_keys.shape[1]
    group_size = H // KVH
    query_heads = queries.reshape(local_rows, KVH, group_size, HD)
    past_keys = cache_keys.reshape(local_rows, cache_span, KVH, HD)
    past_values = cache_values.reshape(local_rows, cache_span, KVH, HD)
    score_scale = 1.0 / math.sqrt(HD)
    past_scores = (
        jnp.einsum("tgqd,tcgd->tgqc", query_heads, past_keys, preferred_element_type=jnp.float32)
        * score_scale
    )
    own_scores = (
        jnp.einsum(
            "tgqd,tgd->tgq",
            query_heads,
            new_keys.reshape(local_rows, KVH, HD),
            preferred_element_type=jnp.float32,
        )
        * score_scale
    )
    is_valid = lax.broadcasted_iota(jnp.int32, (local_rows, cache_span), 1) < cache_len[:, None]
    past_scores = jnp.where(is_valid[:, None, None, :], past_scores, -1e30)
    peak_score = jnp.maximum(jnp.max(past_scores, axis=3), own_scores)
    past_exp = jnp.exp(past_scores - peak_score[..., None])
    own_exp = jnp.exp(own_scores - peak_score)
    denom_sum = jnp.sum(past_exp, axis=3) + own_exp
    past_weights = (past_exp / denom_sum[..., None]).astype(jnp.bfloat16)
    own_weights = (own_exp / denom_sum).astype(jnp.bfloat16)
    blended = jnp.einsum(
        "tgqc,tcgd->tgqd", past_weights, past_values, preferred_element_type=jnp.float32
    )
    blended = blended + own_weights.astype(jnp.float32)[..., None] * new_values.reshape(
        local_rows, KVH, 1, HD
    ).astype(jnp.float32)
    return blended.reshape(local_rows, H * HD).astype(jnp.bfloat16)


def local(
    resid,
    queries,
    new_keys,
    new_values,
    cache_keys,
    cache_values,
    cache_len,
    out_proj,
    norm_gain,
    router,
    expert_ids,
    gate_slab,
    up_slab,
    down_slab,
):
    rows = resid.shape[0]
    chips = lax.axis_size("chip")
    groups = lax.axis_size("chip") * lax.axis_size("core")
    core = lax.axis_index("core")
    half = lax.axis_index("dp") // 2

    other_proj = flipped(out_proj, "core", 1)
    other_down = flipped(down_slab, "dp", 1)
    ids = jnp.concatenate([expert_ids] + [flipped(expert_ids, "dp", m) for m in (3, 1, 2)], axis=0)

    attended = attend(queries, new_keys, new_values, cache_keys, cache_values, cache_len)
    piece = out_proj.shape[0]
    pieces = attended.reshape(rows, chips, 2, piece)
    first = jnp.where(core == 0, pieces[:, :, 0], pieces[:, :, 1])
    second = jnp.where(core == 0, pieces[:, :, 1], pieces[:, :, 0])
    sent = jnp.concatenate([first, second], axis=2).transpose(1, 0, 2)
    regrouped = lax.all_to_all(sent, "chip", split_axis=0, concat_axis=0, tiled=True)
    regrouped = regrouped.reshape(chips * rows, 2 * piece)
    partial = jnp.dot(regrouped[:, :piece], out_proj, preferred_element_type=jnp.float32)
    partial = partial + jnp.dot(
        regrouped[:, piece:], other_proj, preferred_element_type=jnp.float32
    )
    partial = lax.all_to_all(
        partial.astype(jnp.bfloat16).reshape(chips, rows, D),
        "chip",
        split_axis=0,
        concat_axis=0,
        tiled=True,
    )
    hidden = resid.astype(jnp.float32) + jnp.sum(partial.astype(jnp.float32), axis=0)
    meansq = jnp.mean(hidden * hidden, axis=1, keepdims=True)
    normed = (hidden * lax.rsqrt(jnp.maximum(meansq, 0.25)) * norm_gain).astype(jnp.bfloat16)

    mirror = flipped(normed, "dp", 3)
    tokens = jnp.concatenate(
        [normed, mirror, flipped(normed, "dp", 1), flipped(normed, "dp", 2)], axis=0
    )

    count = tokens.shape[0]
    labels = 2 * jnp.arange(groups, dtype=jnp.int32) + half
    hits = ids.T[:, None, :] == labels[None, :, None]
    member = jnp.any(hits, axis=0)
    at = jnp.arange(count, dtype=jnp.int32)
    before = (at[:, None] < at[None, :]) & (at[:, None] // rows == at[None, :] // rows)
    rank = jnp.dot(
        member.astype(jnp.bfloat16),
        before.astype(jnp.bfloat16),
        preferred_element_type=jnp.float32,
    ).astype(jnp.int32)
    place = jnp.where(member, rank + CAP * (at // rows)[None, :], -1)
    slots = CAP * (count // rows)
    dispatch = place[:, None, :] == jnp.arange(slots, dtype=jnp.int32)[None, :, None]
    outgoing = jnp.dot(
        dispatch.reshape(groups * slots, count).astype(jnp.bfloat16),
        tokens,
        preferred_element_type=jnp.float32,
    ).astype(jnp.bfloat16)
    incoming = lax.all_to_all(
        outgoing.reshape(groups, slots, D), EP, split_axis=0, concat_axis=0, tiled=True
    )

    kept = 2 * rows
    logits = jnp.dot(
        jnp.concatenate([normed, mirror], axis=0), router, preferred_element_type=jnp.float32
    )
    experts = router.shape[1]
    onehot = ids[:kept, :, None] == jnp.arange(experts, dtype=jnp.int32)[None, None, :]
    chosen = jnp.sum(jnp.where(onehot, logits[:, None, :], 0.0), axis=2)
    peak_logit = jnp.max(chosen, axis=1, keepdims=True)
    exp_logit = jnp.exp(chosen - peak_logit)
    gate_probs = (exp_logit / jnp.sum(exp_logit, axis=1, keepdims=True)).astype(jnp.bfloat16)
    spread = jnp.sum(
        jnp.where(hits[:, :, :kept], gate_probs.astype(jnp.float32).T[:, None, :], 0.0), axis=0
    )
    back = slots // 2
    combine = jnp.where(
        place[:, None, :kept] == jnp.arange(back, dtype=jnp.int32)[None, :, None],
        spread[:, None, :],
        0.0,
    ).astype(jnp.bfloat16)

    flat = incoming.reshape(groups * slots, D)
    gate_val = jnp.dot(flat, gate_slab[0], preferred_element_type=jnp.float32)
    up_val = jnp.dot(flat, up_slab[0], preferred_element_type=jnp.float32)
    act = (jax.nn.silu(gate_val) * up_val).astype(jnp.bfloat16).reshape(groups, slots, -1)
    other_act = flipped(act[:, back:].reshape(groups * back, -1), "dp", 1)
    produced = jnp.dot(
        act[:, :back].reshape(groups * back, -1), down_slab[0], preferred_element_type=jnp.float32
    )
    produced = produced + jnp.dot(other_act, other_down[0], preferred_element_type=jnp.float32)
    returned = lax.all_to_all(
        produced.astype(jnp.bfloat16).reshape(groups, back, D),
        EP,
        split_axis=0,
        concat_axis=0,
        tiled=True,
    )
    mix = lax.dot_general(
        combine.reshape(groups * back, kept),
        returned.reshape(groups * back, D),
        (((0,), (0,)), ((), ())),
        preferred_element_type=jnp.float32,
    )
    return hidden + mix[:rows] + flipped(mix[rows:], "dp", 3)


def solution(mesh):
    split = Mesh(mesh.devices.reshape(-1, 2, mesh.shape["dp"]), ALL)
    in_specs = (
        P(ALL, None),
        P(ALL, None),
        P(ALL, None),
        P(ALL, None),
        P(ALL, None, None),
        P(ALL, None, None),
        P(ALL),
        P(EP, None),
        P(),
        P(),
        P(ALL, None),
        P(ALL, None, None),
        P(ALL, None, None),
        P(ALL, None, None),
    )
    return jax.shard_map(
        local, mesh=split, in_specs=in_specs, out_specs=P(ALL, None), check_vma=False
    )
```

```python
import math

import jax
import jax.numpy as jnp
from jax import lax
from jax.experimental import pallas as pl
from jax.experimental.pallas import tpu as pltpu
from jax.sharding import Mesh
from jax.sharding import PartitionSpec as P

D = 4096
H = 64
KVH = 4
HD = 128
CAP = 4
ATTN_STEPS = 2
IN_STEPS = 4
OUT_STEPS = 4


EP = ("chip", "core")
ALL = ("chip", "core", "dp")


def flipped(value, axis, mask):
    pairs = [(source, source ^ mask) for source in range(lax.axis_size(axis))]
    return lax.ppermute(value, axis, pairs)


def attention_kernel(swap, lengths, q_in, nk_in, nv_in, keys, values, out, q_buf, o_buf):
    step = pl.program_id(0)
    tokens = q_in.shape[0]
    group = H // KVH
    scale = 1.0 / math.sqrt(HD)

    @pl.when(step == 0)
    def _():
        for head in range(H):
            q_buf[pl.ds(head, tokens, stride=H), :] = q_in[:, head * HD : (head + 1) * HD].astype(
                jnp.float32
            )

    nk = nk_in[...].astype(jnp.float32)
    nv = nv_in[...].astype(jnp.float32)
    span = keys.shape[1]
    owner = lax.broadcasted_iota(jnp.int32, (H, HD), 0) // group
    position = lax.broadcasted_iota(jnp.int32, (H, span), 1)
    for local_row in range(keys.shape[0]):
        row = step * keys.shape[0] + local_row
        q = q_buf[pl.ds(row * H, H), :]
        blocks = [jnp.where(owner == g, q, 0.0).astype(jnp.bfloat16) for g in range(KVH)]
        scores = scale * lax.dot_general(
            jnp.concatenate(blocks, axis=1),
            keys[local_row],
            (((1,), (1,)), ((), ())),
            preferred_element_type=jnp.float32,
        )
        new_key = jnp.concatenate(
            [
                jnp.broadcast_to(nk[local_row : local_row + 1, g * HD : (g + 1) * HD], (group, HD))
                for g in range(KVH)
            ],
            axis=0,
        )
        new_value = jnp.concatenate(
            [
                jnp.broadcast_to(nv[local_row : local_row + 1, g * HD : (g + 1) * HD], (group, HD))
                for g in range(KVH)
            ],
            axis=0,
        )
        own = scale * jnp.sum(q * new_key, axis=1, keepdims=True)
        scores = jnp.where(position < lengths[row], scores, -1e30)
        peak = jnp.maximum(jnp.max(scores, axis=1, keepdims=True), own)
        past_exp = jnp.exp(scores - peak)
        own_exp = jnp.exp(own - peak)
        denom = jnp.sum(past_exp, axis=1, keepdims=True) + own_exp
        weights = (past_exp / denom).astype(jnp.bfloat16)
        own_weight = (own_exp / denom).astype(jnp.bfloat16).astype(jnp.float32)
        wide = jnp.dot(weights, values[local_row], preferred_element_type=jnp.float32)
        blended = jnp.concatenate(
            [wide[g * group : (g + 1) * group, g * HD : (g + 1) * HD] for g in range(KVH)], axis=0
        )
        o_buf[pl.ds(row * H, H), :] = blended + own_weight * new_value

    @pl.when(step == pl.num_programs(0) - 1)
    def _():
        chips, _, width = out.shape
        per = width // HD
        for chip in range(chips):
            for at in range(per):
                head = chip * per + at
                first = o_buf[pl.ds(head, tokens, stride=H), :]
                second = o_buf[pl.ds(chip * per + (at ^ (per // 2)), tokens, stride=H), :]
                out[chip, :, at * HD : (at + 1) * HD] = jnp.where(
                    swap[0] == 1, second, first
                ).astype(jnp.bfloat16)


def attention(swap, queries, new_keys, new_values, cache_keys, cache_values, cache_len, chips):
    rows = queries.shape[0]
    span = cache_keys.shape[1]
    each = rows // ATTN_STEPS
    smem = pl.BlockSpec(memory_space=pltpu.SMEM)
    return pl.pallas_call(
        attention_kernel,
        grid=(ATTN_STEPS,),
        out_shape=jax.ShapeDtypeStruct((chips, rows, H * HD // chips), jnp.bfloat16),
        in_specs=[
            smem,
            smem,
            pl.BlockSpec((rows, H * HD), lambda i: (0, 0)),
            pl.BlockSpec((each, KVH * HD), lambda i: (i, 0)),
            pl.BlockSpec((each, KVH * HD), lambda i: (i, 0)),
            pl.BlockSpec((each, span, KVH * HD), lambda i: (i, 0, 0)),
            pl.BlockSpec((each, span, KVH * HD), lambda i: (i, 0, 0)),
        ],
        out_specs=pl.BlockSpec((chips, rows, H * HD // chips), lambda i: (0, 0, 0)),
        scratch_shapes=[
            pltpu.VMEM((rows * H, HD), jnp.float32),
            pltpu.VMEM((rows * H, HD), jnp.float32),
        ],
        compiler_params=pltpu.CompilerParams(dimension_semantics=("arbitrary",)),
        cost_estimate=pl.CostEstimate(
            flops=8 * rows * H * HD * span, bytes_accessed=4 * rows * span * KVH * HD, transcendentals=0
        ),
        name="attention",
    )(swap, cache_len, queries, new_keys, new_values, cache_keys, cache_values)


def start_slabs(flag, own, crossed, near, far, start):
    @pl.when(flag[0] == 1)
    def _():
        start(0, own)
        start(1, crossed)

    @pl.when(flag[0] != 1)
    def _():
        start(0, near)
        start(1, far)


def act_kernel(flag, rows_in, *refs):
    own, crossed, near, far = refs[0:2], refs[2:4], refs[4:6], refs[6:8]
    out, x_buf, in_buf, x_sem, in_sem = refs[8:]
    hf = own[0].shape[2]
    span = D // IN_STEPS

    def copy(side, source, step, part):
        return pltpu.make_async_copy(
            source[part].at[0, pl.ds(step * span, span)],
            in_buf.at[side, pl.ds(step * span, span), pl.ds(part * hf, hf)],
            in_sem.at[side, step, part],
        )

    def start(side, source):
        for step in range(IN_STEPS):
            for part in range(2):
                copy(side, source, step, part).start()

    x_copy = pltpu.make_async_copy(rows_in, x_buf, x_sem)
    x_copy.start()
    start_slabs(flag, own, crossed, near, far, start)
    x_copy.wait()
    for side in range(2):
        total = None
        for step in range(IN_STEPS):
            for part in range(2):
                copy(side, own, step, part).wait()
            piece = jnp.dot(
                x_buf[:, step * span : (step + 1) * span],
                in_buf[side, step * span : (step + 1) * span],
                preferred_element_type=jnp.float32,
            )
            total = piece if total is None else total + piece
        gate_val = total[:, :hf]
        out[:, side * hf : (side + 1) * hf] = (
            gate_val / (1.0 + jnp.exp(-gate_val)) * total[:, hf:]
        ).astype(jnp.bfloat16)


def down_kernel(flag, act, own, crossed, near, far, out, buf, sem):
    hf = own.shape[1]
    wide = D // OUT_STEPS

    def copy(side, source, step):
        return pltpu.make_async_copy(
            source.at[0, :, pl.ds(step * wide, wide)],
            buf.at[pl.ds(side * hf, hf), pl.ds(step * wide, wide)],
            sem.at[side, step],
        )

    def start(side, source):
        for step in range(OUT_STEPS):
            copy(side, source, step).start()

    start_slabs(flag, own, crossed, near, far, start)
    for step in range(OUT_STEPS):
        for side in range(2):
            copy(side, own, step).wait()
        out[:, step * wide : (step + 1) * wide] = jnp.dot(
            act[...],
            buf[:, step * wide : (step + 1) * wide],
            preferred_element_type=jnp.float32,
        ).astype(jnp.bfloat16)


def expert_act(flag, rows_in, own, crossed, near, far):
    count = rows_in.shape[0]
    hf = own[0].shape[2]
    return pl.pallas_call(
        act_kernel,
        out_shape=jax.ShapeDtypeStruct((count, 2 * hf), jnp.bfloat16),
        in_specs=[pl.BlockSpec(memory_space=pltpu.SMEM)]
        + [pl.BlockSpec(memory_space=pltpu.HBM)] * 9,
        out_specs=pl.BlockSpec(memory_space=pltpu.VMEM),
        scratch_shapes=[
            pltpu.VMEM((count, D), jnp.bfloat16),
            pltpu.VMEM((2, D, 2 * hf), jnp.bfloat16),
            pltpu.SemaphoreType.DMA,
            pltpu.SemaphoreType.DMA((2, IN_STEPS, 2)),
        ],
        compiler_params=pltpu.CompilerParams(vmem_limit_bytes=28 * 1024 * 1024),
        cost_estimate=pl.CostEstimate(
            flops=8 * count * D * hf, bytes_accessed=8 * D * hf + 2 * count * D, transcendentals=0
        ),
        name="expert_act",
    )(flag, rows_in, *own, *crossed, *near, *far)


def expert_down(flag, act, own, crossed, near, far):
    count = act.shape[0]
    hf = own.shape[1]
    return pl.pallas_call(
        down_kernel,
        out_shape=jax.ShapeDtypeStruct((count, D), jnp.bfloat16),
        in_specs=[pl.BlockSpec(memory_space=pltpu.SMEM), pl.BlockSpec(memory_space=pltpu.VMEM)]
        + [pl.BlockSpec(memory_space=pltpu.HBM)] * 4,
        out_specs=pl.BlockSpec(memory_space=pltpu.VMEM),
        scratch_shapes=[
            pltpu.VMEM((2 * hf, D), jnp.bfloat16),
            pltpu.SemaphoreType.DMA((2, OUT_STEPS)),
        ],
        compiler_params=pltpu.CompilerParams(vmem_limit_bytes=20 * 1024 * 1024),
        cost_estimate=pl.CostEstimate(
            flops=4 * count * D * hf, bytes_accessed=4 * D * hf + 2 * count * D, transcendentals=0
        ),
        name="expert_down",
    )(flag, act, own, crossed, near, far)


def local(
    resid,
    queries,
    new_keys,
    new_values,
    cache_keys,
    cache_values,
    cache_len,
    out_proj,
    norm_gain,
    router,
    expert_ids,
    gate_slab,
    up_slab,
    down_slab,
):
    rows = resid.shape[0]
    chips = lax.axis_size("chip")
    core = lax.axis_index("core")
    depth = lax.axis_index("dp")
    depths = lax.axis_size("dp")

    other_proj = flipped(out_proj, "core", 1)
    places = [(c, d) for c in range(2) for d in range(depths)]
    across = [(c * depths + d, c * depths + (d ^ 1)) for c, d in places if c != d % 2]
    beside = [(c * depths + d, (1 - c) * depths + d) for c, d in places if c == d % 2]

    def spread_out(slab):
        crossed = lax.ppermute(slab, ("core", "dp"), across)
        return crossed, lax.ppermute(slab, ("core", "dp"), beside)

    def shared(slab, after):
        held, _ = lax.optimization_barrier((slab, after))
        return lax.ppermute(held, ("core", "dp"), beside)

    gate_crossed, gate_near = spread_out(gate_slab)
    up_crossed, up_near = spread_out(up_slab)
    down_crossed, down_near = spread_out(down_slab)
    flag = (core == depth % 2).astype(jnp.int32).reshape(1)
    ids = jnp.concatenate([expert_ids] + [flipped(expert_ids, "dp", m) for m in (1, 2, 3)], axis=0)

    piece = out_proj.shape[0]
    sent = attention(
        core.astype(jnp.int32).reshape(1),
        queries,
        new_keys,
        new_values,
        cache_keys,
        cache_values,
        cache_len,
        chips,
    )
    regrouped = lax.all_to_all(sent, "chip", split_axis=0, concat_axis=0, tiled=True)
    regrouped = regrouped.reshape(chips * rows, 2 * piece)
    partial = jnp.dot(regrouped[:, :piece], out_proj, preferred_element_type=jnp.float32)
    partial = partial + jnp.dot(
        regrouped[:, piece:], other_proj, preferred_element_type=jnp.float32
    )
    partial = partial.astype(jnp.bfloat16)
    gate_far = shared(gate_crossed, partial)
    partial = lax.all_to_all(
        partial.reshape(chips, rows, D),
        "chip",
        split_axis=0,
        concat_axis=0,
        tiled=True,
    )
    hidden = resid.astype(jnp.float32) + jnp.sum(partial.astype(jnp.float32), axis=0)
    meansq = jnp.mean(hidden * hidden, axis=1, keepdims=True)
    normed = (hidden * lax.rsqrt(jnp.maximum(meansq, 0.25)) * norm_gain).astype(jnp.bfloat16)

    tokens = jnp.concatenate([normed] + [flipped(normed, "dp", m) for m in (1, 2, 3)], axis=0)

    count = tokens.shape[0]
    labels = 4 * jnp.arange(chips, dtype=jnp.int32) + 2 * (depth % 2) + depth // 2
    hits = ids.T[:, None, :] == labels[None, :, None]
    member = jnp.any(hits, axis=0)
    at = jnp.arange(count, dtype=jnp.int32)
    before = (at[:, None] < at[None, :]) & (at[:, None] // rows == at[None, :] // rows)
    rank = jnp.dot(
        member.astype(jnp.bfloat16),
        before.astype(jnp.bfloat16),
        preferred_element_type=jnp.float32,
    ).astype(jnp.int32)
    place = jnp.where(member, rank + CAP * (at // rows)[None, :], -1)
    slots = CAP * depths
    dispatch = place[:, None, :] == jnp.arange(slots, dtype=jnp.int32)[None, :, None]
    outgoing = jnp.dot(
        dispatch.reshape(chips * slots, count).astype(jnp.bfloat16),
        tokens,
        preferred_element_type=jnp.float32,
    ).astype(jnp.bfloat16)
    up_far = shared(up_crossed, outgoing)
    incoming = lax.all_to_all(
        outgoing.reshape(chips, slots, D), "chip", split_axis=0, concat_axis=0, tiled=True
    )

    logits = jnp.dot(tokens, router, preferred_element_type=jnp.float32)
    experts = router.shape[1]
    onehot = ids[:, :, None] == jnp.arange(experts, dtype=jnp.int32)[None, None, :]
    chosen = jnp.sum(jnp.where(onehot, logits[:, None, :], 0.0), axis=2)
    peak_logit = jnp.max(chosen, axis=1, keepdims=True)
    exp_logit = jnp.exp(chosen - peak_logit)
    gate_probs = (exp_logit / jnp.sum(exp_logit, axis=1, keepdims=True)).astype(jnp.bfloat16)
    spread = jnp.sum(
        jnp.where(hits, gate_probs.astype(jnp.float32).T[:, None, :], 0.0), axis=0
    )
    combine = jnp.where(dispatch, spread[:, None, :], 0.0).astype(jnp.bfloat16)

    down_far = shared(down_crossed, incoming)
    act = expert_act(
        flag,
        incoming.reshape(chips * slots, D),
        (gate_slab, up_slab),
        (gate_crossed, up_crossed),
        (gate_near, up_near),
        (gate_far, up_far),
    )
    produced = expert_down(flag, act, down_slab, down_crossed, down_near, down_far)
    returned = lax.all_to_all(
        produced.reshape(chips, slots, D), "chip", split_axis=0, concat_axis=0, tiled=True
    )
    mix = lax.dot_general(
        combine.reshape(chips * slots, count),
        returned.reshape(chips * slots, D),
        (((0,), (0,)), ((), ())),
        preferred_element_type=jnp.float32,
    )
    total = hidden + mix[:rows]
    narrow = mix.astype(jnp.bfloat16)
    for m in (1, 2, 3):
        total = total + flipped(narrow[m * rows : (m + 1) * rows], "dp", m).astype(jnp.float32)
    return total


def solution(mesh):
    split = Mesh(mesh.devices.reshape(-1, 2, mesh.shape["dp"]), ALL)
    in_specs = (
        P(ALL, None),
        P(ALL, None),
        P(ALL, None),
        P(ALL, None),
        P(ALL, None, None),
        P(ALL, None, None),
        P(ALL),
        P(EP, None),
        P(),
        P(),
        P(ALL, None),
        P(ALL, None, None),
        P(ALL, None, None),
        P(ALL, None, None),
    )

    return jax.shard_map(
        local, mesh=split, in_specs=in_specs, out_specs=P(ALL, None), check_vma=False
    )
```

```python
import math

import jax
import jax.numpy as jnp
from jax import lax
from jax.experimental import pallas as pl
from jax.experimental.pallas import tpu as pltpu
from jax.sharding import Mesh
from jax.sharding import PartitionSpec as P

D = 4096
H = 64
KVH = 4
HD = 128
CAP = 4
ATTN_STEPS = 2
OUT_STEPS = 4


EP = ("chip", "core")
ALL = ("chip", "core", "dp")


def flipped(value, axis, mask):
    pairs = [(source, source ^ mask) for source in range(lax.axis_size(axis))]
    return lax.ppermute(value, axis, pairs)


def attention_kernel(swap, lengths, q_in, nk_in, nv_in, keys, values, out, q_buf, o_buf):
    step = pl.program_id(0)
    tokens = q_in.shape[0]
    group = H // KVH
    scale = 1.0 / math.sqrt(HD)

    @pl.when(step == 0)
    def _():
        for head in range(H):
            q_buf[pl.ds(head, tokens, stride=H), :] = q_in[:, head * HD : (head + 1) * HD].astype(
                jnp.float32
            )

    nk = nk_in[...].astype(jnp.float32)
    nv = nv_in[...].astype(jnp.float32)
    span = keys.shape[1]
    owner = lax.broadcasted_iota(jnp.int32, (H, HD), 0) // group
    position = lax.broadcasted_iota(jnp.int32, (H, span), 1)
    for local_row in range(keys.shape[0]):
        row = step * keys.shape[0] + local_row
        q = q_buf[pl.ds(row * H, H), :]
        blocks = [jnp.where(owner == g, q, 0.0).astype(jnp.bfloat16) for g in range(KVH)]
        scores = scale * lax.dot_general(
            jnp.concatenate(blocks, axis=1),
            keys[local_row],
            (((1,), (1,)), ((), ())),
            preferred_element_type=jnp.float32,
        )
        new_key = jnp.concatenate(
            [
                jnp.broadcast_to(nk[local_row : local_row + 1, g * HD : (g + 1) * HD], (group, HD))
                for g in range(KVH)
            ],
            axis=0,
        )
        new_value = jnp.concatenate(
            [
                jnp.broadcast_to(nv[local_row : local_row + 1, g * HD : (g + 1) * HD], (group, HD))
                for g in range(KVH)
            ],
            axis=0,
        )
        own = scale * jnp.sum(q * new_key, axis=1, keepdims=True)
        scores = jnp.where(position < lengths[row], scores, -1e30)
        peak = jnp.maximum(jnp.max(scores, axis=1, keepdims=True), own)
        past_exp = jnp.exp(scores - peak)
        own_exp = jnp.exp(own - peak)
        denom = jnp.sum(past_exp, axis=1, keepdims=True) + own_exp
        weights = (past_exp / denom).astype(jnp.bfloat16)
        own_weight = (own_exp / denom).astype(jnp.bfloat16).astype(jnp.float32)
        wide = jnp.dot(weights, values[local_row], preferred_element_type=jnp.float32)
        blended = jnp.concatenate(
            [wide[g * group : (g + 1) * group, g * HD : (g + 1) * HD] for g in range(KVH)], axis=0
        )
        o_buf[pl.ds(row * H, H), :] = blended + own_weight * new_value

    @pl.when(step == pl.num_programs(0) - 1)
    def _():
        chips, _, width = out.shape
        per = width // HD
        for chip in range(chips):
            for at in range(per):
                head = chip * per + at
                first = o_buf[pl.ds(head, tokens, stride=H), :]
                second = o_buf[pl.ds(chip * per + (at ^ (per // 2)), tokens, stride=H), :]
                out[chip, :, at * HD : (at + 1) * HD] = jnp.where(
                    swap[0] == 1, second, first
                ).astype(jnp.bfloat16)


def attention(swap, queries, new_keys, new_values, cache_keys, cache_values, cache_len, chips):
    rows = queries.shape[0]
    span = cache_keys.shape[1]
    each = rows // ATTN_STEPS
    smem = pl.BlockSpec(memory_space=pltpu.SMEM)
    return pl.pallas_call(
        attention_kernel,
        grid=(ATTN_STEPS,),
        out_shape=jax.ShapeDtypeStruct((chips, rows, H * HD // chips), jnp.bfloat16),
        in_specs=[
            smem,
            smem,
            pl.BlockSpec((rows, H * HD), lambda i: (0, 0)),
            pl.BlockSpec((each, KVH * HD), lambda i: (i, 0)),
            pl.BlockSpec((each, KVH * HD), lambda i: (i, 0)),
            pl.BlockSpec((each, span, KVH * HD), lambda i: (i, 0, 0)),
            pl.BlockSpec((each, span, KVH * HD), lambda i: (i, 0, 0)),
        ],
        out_specs=pl.BlockSpec((chips, rows, H * HD // chips), lambda i: (0, 0, 0)),
        scratch_shapes=[
            pltpu.VMEM((rows * H, HD), jnp.float32),
            pltpu.VMEM((rows * H, HD), jnp.float32),
        ],
        compiler_params=pltpu.CompilerParams(dimension_semantics=("arbitrary",)),
        cost_estimate=pl.CostEstimate(
            flops=8 * rows * H * HD * span, bytes_accessed=4 * rows * span * KVH * HD, transcendentals=0
        ),
        name="attention",
    )(swap, cache_len, queries, new_keys, new_values, cache_keys, cache_values)


def start_slabs(flag, own, crossed, near, far, start):
    @pl.when(flag[0] == 1)
    def _():
        start(0, own)
        start(1, crossed)

    @pl.when(flag[0] != 1)
    def _():
        start(0, near)
        start(1, far)


def act_kernel(flag, rows_in, *refs):
    own, crossed, near, far = refs[0:2], refs[2:4], refs[4:6], refs[6:8]
    out, x_buf, buf, x_sem, sem = refs[8:]
    hf = own[0].shape[2]

    def copy(side, source, part):
        return pltpu.make_async_copy(
            source[part].at[0], buf.at[2 * side + part], sem.at[2 * side + part]
        )

    def start(side, source):
        for part in range(2):
            copy(side, source, part).start()

    x_copy = pltpu.make_async_copy(rows_in, x_buf, x_sem)
    x_copy.start()
    start_slabs(flag, own, crossed, near, far, start)
    x_copy.wait()
    for side in range(2):
        vals = []
        for part in range(2):
            copy(side, own, part).wait()
            vals.append(
                jnp.dot(x_buf[...], buf[2 * side + part], preferred_element_type=jnp.float32)
            )
        gate_val, up_val = vals
        out[:, side * hf : (side + 1) * hf] = (
            gate_val / (1.0 + jnp.exp(-gate_val)) * up_val
        ).astype(jnp.bfloat16)


def down_kernel(flag, act, own, crossed, near, far, out, buf, sem):
    hf = own.shape[1]
    wide = D // OUT_STEPS

    def copy(side, source, step):
        return pltpu.make_async_copy(
            source.at[0, :, pl.ds(step * wide, wide)],
            buf.at[pl.ds(side * hf, hf), pl.ds(step * wide, wide)],
            sem.at[side, step],
        )

    def start(side, source):
        for step in range(OUT_STEPS):
            copy(side, source, step).start()

    start_slabs(flag, own, crossed, near, far, start)
    for step in range(OUT_STEPS):
        for side in range(2):
            copy(side, own, step).wait()
        out[:, step * wide : (step + 1) * wide] = jnp.dot(
            act[...],
            buf[:, step * wide : (step + 1) * wide],
            preferred_element_type=jnp.float32,
        ).astype(jnp.bfloat16)


def expert_act(flag, rows_in, own, crossed, near, far):
    count = rows_in.shape[0]
    hf = own[0].shape[2]
    return pl.pallas_call(
        act_kernel,
        out_shape=jax.ShapeDtypeStruct((count, 2 * hf), jnp.bfloat16),
        in_specs=[pl.BlockSpec(memory_space=pltpu.SMEM)]
        + [pl.BlockSpec(memory_space=pltpu.HBM)] * 9,
        out_specs=pl.BlockSpec(memory_space=pltpu.VMEM),
        scratch_shapes=[
            pltpu.VMEM((count, D), jnp.bfloat16),
            pltpu.VMEM((4, D, hf), jnp.bfloat16),
            pltpu.SemaphoreType.DMA,
            pltpu.SemaphoreType.DMA((4,)),
        ],
        compiler_params=pltpu.CompilerParams(vmem_limit_bytes=123 * 512 * 1024),
        cost_estimate=pl.CostEstimate(
            flops=8 * count * D * hf, bytes_accessed=8 * D * hf + 2 * count * D, transcendentals=0
        ),
        name="expert_act",
    )(flag, rows_in, *own, *crossed, *near, *far)


def expert_down(flag, act, own, crossed, near, far):
    count = act.shape[0]
    hf = own.shape[1]
    return pl.pallas_call(
        down_kernel,
        out_shape=jax.ShapeDtypeStruct((count, D), jnp.bfloat16),
        in_specs=[pl.BlockSpec(memory_space=pltpu.SMEM), pl.BlockSpec(memory_space=pltpu.VMEM)]
        + [pl.BlockSpec(memory_space=pltpu.HBM)] * 4,
        out_specs=pl.BlockSpec(memory_space=pltpu.VMEM),
        scratch_shapes=[
            pltpu.VMEM((2 * hf, D), jnp.bfloat16),
            pltpu.SemaphoreType.DMA((2, OUT_STEPS)),
        ],
        compiler_params=pltpu.CompilerParams(vmem_limit_bytes=20 * 1024 * 1024),
        cost_estimate=pl.CostEstimate(
            flops=4 * count * D * hf, bytes_accessed=4 * D * hf + 2 * count * D, transcendentals=0
        ),
        name="expert_down",
    )(flag, act, own, crossed, near, far)


def local(
    resid,
    queries,
    new_keys,
    new_values,
    cache_keys,
    cache_values,
    cache_len,
    out_proj,
    norm_gain,
    router,
    expert_ids,
    gate_slab,
    up_slab,
    down_slab,
):
    rows = resid.shape[0]
    chips = lax.axis_size("chip")
    core = lax.axis_index("core")
    depth = lax.axis_index("dp")
    depths = lax.axis_size("dp")

    other_proj = flipped(out_proj, "core", 1)
    places = [(c, d) for c in range(2) for d in range(depths)]
    across = [(c * depths + d, c * depths + (d ^ 1)) for c, d in places if c != d % 2]
    beside = [(c * depths + d, (1 - c) * depths + d) for c, d in places if c == d % 2]

    def moved(slab, pairs, after=None):
        if after is not None:
            slab, _ = lax.optimization_barrier((slab, after))
        return lax.ppermute(slab, ("core", "dp"), pairs)

    gate_crossed = moved(gate_slab, across)
    gate_near = moved(gate_slab, beside)
    up_near = moved(up_slab, beside)
    down_near = moved(down_slab, beside)
    flag = (core == depth % 2).astype(jnp.int32).reshape(1)
    other_ids = [flipped(expert_ids, "dp", m) for m in (1, 2, 3)]
    ids = jnp.concatenate([expert_ids] + other_ids, axis=0)

    piece = out_proj.shape[0]
    sent = attention(
        core.astype(jnp.int32).reshape(1),
        queries,
        new_keys,
        new_values,
        cache_keys,
        cache_values,
        cache_len,
        chips,
    )
    regrouped = lax.all_to_all(sent, "chip", split_axis=0, concat_axis=0, tiled=True)
    regrouped = regrouped.reshape(chips * rows, 2 * piece)
    partial = jnp.dot(regrouped[:, :piece], out_proj, preferred_element_type=jnp.float32)
    partial = partial + jnp.dot(
        regrouped[:, piece:], other_proj, preferred_element_type=jnp.float32
    )
    count = ids.shape[0]
    labels = 4 * jnp.arange(chips, dtype=jnp.int32) + 2 * (depth % 2) + depth // 2
    hits = ids.T[:, None, :] == labels[None, :, None]
    member = jnp.any(hits, axis=0)
    at = jnp.arange(count, dtype=jnp.int32)
    before = (at[:, None] < at[None, :]) & (at[:, None] // rows == at[None, :] // rows)
    rank = jnp.dot(
        member.astype(jnp.bfloat16),
        before.astype(jnp.bfloat16),
        preferred_element_type=jnp.float32,
    ).astype(jnp.int32)
    place = jnp.where(member, rank + CAP * (at // rows)[None, :], -1)
    slots = CAP * depths
    dispatch = place[:, None, :] == jnp.arange(slots, dtype=jnp.int32)[None, :, None]

    partial = partial.astype(jnp.bfloat16)
    gate_far = moved(gate_crossed, beside, partial)
    up_crossed = moved(up_slab, across, partial)
    partial = lax.all_to_all(
        partial.reshape(chips, rows, D),
        "chip",
        split_axis=0,
        concat_axis=0,
        tiled=True,
    )
    partial, dispatch = lax.optimization_barrier((partial, dispatch))
    hidden = resid.astype(jnp.float32) + jnp.sum(partial.astype(jnp.float32), axis=0)
    meansq = jnp.mean(hidden * hidden, axis=1, keepdims=True)
    normed = (hidden * lax.rsqrt(jnp.maximum(meansq, 0.25)) * norm_gain).astype(jnp.bfloat16)

    others = [flipped(normed, "dp", m) for m in (1, 2, 3)]
    tokens = jnp.concatenate([normed] + others, axis=0)
    down_crossed = moved(down_slab, across, others)

    outgoing = jnp.dot(
        dispatch.reshape(chips * slots, count).astype(jnp.bfloat16),
        tokens,
        preferred_element_type=jnp.float32,
    ).astype(jnp.bfloat16)
    up_far = moved(up_crossed, beside, outgoing)
    incoming = lax.all_to_all(
        outgoing.reshape(chips, slots, D), "chip", split_axis=0, concat_axis=0, tiled=True
    )

    logits = jnp.dot(tokens, router, preferred_element_type=jnp.float32)
    experts = router.shape[1]
    onehot = ids[:, :, None] == jnp.arange(experts, dtype=jnp.int32)[None, None, :]
    chosen = jnp.sum(jnp.where(onehot, logits[:, None, :], 0.0), axis=2)
    peak_logit = jnp.max(chosen, axis=1, keepdims=True)
    exp_logit = jnp.exp(chosen - peak_logit)
    gate_probs = (exp_logit / jnp.sum(exp_logit, axis=1, keepdims=True)).astype(jnp.bfloat16)
    spread = jnp.sum(
        jnp.where(hits, gate_probs.astype(jnp.float32).T[:, None, :], 0.0), axis=0
    )
    combine = jnp.where(dispatch, spread[:, None, :], 0.0).astype(jnp.bfloat16)

    down_far = moved(down_crossed, beside, incoming)
    act = expert_act(
        flag,
        incoming.reshape(chips * slots, D),
        (gate_slab, up_slab),
        (gate_crossed, up_crossed),
        (gate_near, up_near),
        (gate_far, up_far),
    )
    produced = expert_down(flag, act, down_slab, down_crossed, down_near, down_far)
    returned = lax.all_to_all(
        produced.reshape(chips, slots, D), "chip", split_axis=0, concat_axis=0, tiled=True
    )
    mix = lax.dot_general(
        combine.reshape(chips * slots, count),
        returned.reshape(chips * slots, D),
        (((0,), (0,)), ((), ())),
        preferred_element_type=jnp.float32,
    )
    total = hidden + mix[:rows]
    narrow = mix.astype(jnp.bfloat16)
    for m in (1, 2, 3):
        total = total + flipped(narrow[m * rows : (m + 1) * rows], "dp", m).astype(jnp.float32)
    return total


def solution(mesh):
    split = Mesh(mesh.devices.reshape(-1, 2, mesh.shape["dp"]), ALL)
    in_specs = (
        P(ALL, None),
        P(ALL, None),
        P(ALL, None),
        P(ALL, None),
        P(ALL, None, None),
        P(ALL, None, None),
        P(ALL),
        P(EP, None),
        P(),
        P(),
        P(ALL, None),
        P(ALL, None, None),
        P(ALL, None, None),
        P(ALL, None, None),
    )

    return jax.shard_map(
        local, mesh=split, in_specs=in_specs, out_specs=P(ALL, None), check_vma=False
    )
```

```python
import math

import jax
import jax.numpy as jnp
from jax import lax
from jax.experimental import pallas as pl
from jax.experimental.pallas import tpu as pltpu
from jax.sharding import Mesh
from jax.sharding import PartitionSpec as P

D = 4096
H = 64
KVH = 4
HD = 128
CAP = 4
ATTN_STEPS = 2
OUT_STEPS = 4


EP = ("chip", "core")
ALL = ("chip", "core", "dp")


def flipped(value, axis, mask):
    pairs = [(source, source ^ mask) for source in range(lax.axis_size(axis))]
    return lax.ppermute(value, axis, pairs)


def attention_kernel(swap, lengths, q_in, nk_in, nv_in, keys, values, out, q_buf, o_buf):
    step = pl.program_id(0)
    tokens = q_in.shape[0]
    group = H // KVH
    scale = 1.0 / math.sqrt(HD)

    @pl.when(step == 0)
    def _():
        for head in range(H):
            q_buf[pl.ds(head, tokens, stride=H), :] = q_in[:, head * HD : (head + 1) * HD].astype(
                jnp.float32
            )

    nk = nk_in[...].astype(jnp.float32)
    nv = nv_in[...].astype(jnp.float32)
    span = keys.shape[1]
    owner = lax.broadcasted_iota(jnp.int32, (H, HD), 0) // group
    position = lax.broadcasted_iota(jnp.int32, (H, span), 1)
    for local_row in range(keys.shape[0]):
        row = step * keys.shape[0] + local_row
        q = q_buf[pl.ds(row * H, H), :]
        blocks = [jnp.where(owner == g, q, 0.0).astype(jnp.bfloat16) for g in range(KVH)]
        scores = scale * lax.dot_general(
            jnp.concatenate(blocks, axis=1),
            keys[local_row],
            (((1,), (1,)), ((), ())),
            preferred_element_type=jnp.float32,
        )
        new_key = jnp.concatenate(
            [
                jnp.broadcast_to(nk[local_row : local_row + 1, g * HD : (g + 1) * HD], (group, HD))
                for g in range(KVH)
            ],
            axis=0,
        )
        new_value = jnp.concatenate(
            [
                jnp.broadcast_to(nv[local_row : local_row + 1, g * HD : (g + 1) * HD], (group, HD))
                for g in range(KVH)
            ],
            axis=0,
        )
        own = scale * jnp.sum(q * new_key, axis=1, keepdims=True)
        scores = jnp.where(position < lengths[row], scores, -1e30)
        peak = jnp.maximum(jnp.max(scores, axis=1, keepdims=True), own)
        past_exp = jnp.exp(scores - peak)
        own_exp = jnp.exp(own - peak)
        denom = jnp.sum(past_exp, axis=1, keepdims=True) + own_exp
        weights = (past_exp / denom).astype(jnp.bfloat16)
        own_weight = (own_exp / denom).astype(jnp.bfloat16).astype(jnp.float32)
        wide = jnp.dot(weights, values[local_row], preferred_element_type=jnp.float32)
        blended = jnp.concatenate(
            [wide[g * group : (g + 1) * group, g * HD : (g + 1) * HD] for g in range(KVH)], axis=0
        )
        o_buf[pl.ds(row * H, H), :] = blended + own_weight * new_value

    @pl.when(step == pl.num_programs(0) - 1)
    def _():
        chips, _, width = out.shape
        per = width // HD
        for chip in range(chips):
            for at in range(per):
                head = chip * per + at
                first = o_buf[pl.ds(head, tokens, stride=H), :]
                second = o_buf[pl.ds(chip * per + (at ^ (per // 2)), tokens, stride=H), :]
                out[chip, :, at * HD : (at + 1) * HD] = jnp.where(
                    swap[0] == 1, second, first
                ).astype(jnp.bfloat16)


def attention(swap, queries, new_keys, new_values, cache_keys, cache_values, cache_len, chips):
    rows = queries.shape[0]
    span = cache_keys.shape[1]
    each = rows // ATTN_STEPS
    smem = pl.BlockSpec(memory_space=pltpu.SMEM)
    return pl.pallas_call(
        attention_kernel,
        grid=(ATTN_STEPS,),
        out_shape=jax.ShapeDtypeStruct((chips, rows, H * HD // chips), jnp.bfloat16),
        in_specs=[
            smem,
            smem,
            pl.BlockSpec((rows, H * HD), lambda i: (0, 0)),
            pl.BlockSpec((each, KVH * HD), lambda i: (i, 0)),
            pl.BlockSpec((each, KVH * HD), lambda i: (i, 0)),
            pl.BlockSpec((each, span, KVH * HD), lambda i: (i, 0, 0)),
            pl.BlockSpec((each, span, KVH * HD), lambda i: (i, 0, 0)),
        ],
        out_specs=pl.BlockSpec((chips, rows, H * HD // chips), lambda i: (0, 0, 0)),
        scratch_shapes=[
            pltpu.VMEM((rows * H, HD), jnp.float32),
            pltpu.VMEM((rows * H, HD), jnp.float32),
        ],
        compiler_params=pltpu.CompilerParams(dimension_semantics=("arbitrary",)),
        cost_estimate=pl.CostEstimate(
            flops=8 * rows * H * HD * span, bytes_accessed=4 * rows * span * KVH * HD, transcendentals=0
        ),
        name="attention",
    )(swap, cache_len, queries, new_keys, new_values, cache_keys, cache_values)


def start_slabs(flag, own, crossed, near, far, start):
    @pl.when(flag[0] == 1)
    def _():
        start(0, own)
        start(1, crossed)

    @pl.when(flag[0] != 1)
    def _():
        start(0, near)
        start(1, far)


def act_kernel(flag, rows_in, *refs):
    own, crossed, near, far = refs[0:2], refs[2:4], refs[4:6], refs[6:8]
    out, x_buf, buf, x_sem, sem = refs[8:]
    hf = own[0].shape[2]

    def copy(side, source, part):
        return pltpu.make_async_copy(
            source[part].at[0], buf.at[2 * side + part], sem.at[2 * side + part]
        )

    def start(side, source):
        for part in range(2):
            copy(side, source, part).start()

    x_copy = pltpu.make_async_copy(rows_in, x_buf, x_sem)
    x_copy.start()
    start_slabs(flag, own, crossed, near, far, start)
    x_copy.wait()
    for side in range(2):
        vals = []
        for part in range(2):
            copy(side, own, part).wait()
            vals.append(
                jnp.dot(x_buf[...], buf[2 * side + part], preferred_element_type=jnp.float32)
            )
        gate_val, up_val = vals
        out[:, side * hf : (side + 1) * hf] = (
            gate_val / (1.0 + jnp.exp(-gate_val)) * up_val
        ).astype(jnp.bfloat16)


def down_kernel(flag, act, own, crossed, near, far, out, buf, sem):
    hf = own.shape[1]
    wide = D // OUT_STEPS

    def copy(side, source, step):
        return pltpu.make_async_copy(
            source.at[0, :, pl.ds(step * wide, wide)],
            buf.at[pl.ds(side * hf, hf), pl.ds(step * wide, wide)],
            sem.at[side, step],
        )

    def start(side, source):
        for step in range(OUT_STEPS):
            copy(side, source, step).start()

    start_slabs(flag, own, crossed, near, far, start)
    for step in range(OUT_STEPS):
        for side in range(2):
            copy(side, own, step).wait()
        out[:, step * wide : (step + 1) * wide] = jnp.dot(
            act[...],
            buf[:, step * wide : (step + 1) * wide],
            preferred_element_type=jnp.float32,
        ).astype(jnp.bfloat16)


def expert_act(flag, rows_in, own, crossed, near, far):
    count = rows_in.shape[0]
    hf = own[0].shape[2]
    return pl.pallas_call(
        act_kernel,
        out_shape=jax.ShapeDtypeStruct((count, 2 * hf), jnp.bfloat16),
        in_specs=[pl.BlockSpec(memory_space=pltpu.SMEM)]
        + [pl.BlockSpec(memory_space=pltpu.HBM)] * 9,
        out_specs=pl.BlockSpec(memory_space=pltpu.VMEM),
        scratch_shapes=[
            pltpu.VMEM((count, D), jnp.bfloat16),
            pltpu.VMEM((4, D, hf), jnp.bfloat16),
            pltpu.SemaphoreType.DMA,
            pltpu.SemaphoreType.DMA((4,)),
        ],
        compiler_params=pltpu.CompilerParams(vmem_limit_bytes=123 * 512 * 1024),
        cost_estimate=pl.CostEstimate(
            flops=8 * count * D * hf, bytes_accessed=8 * D * hf + 2 * count * D, transcendentals=0
        ),
        name="expert_act",
    )(flag, rows_in, *own, *crossed, *near, *far)


def expert_down(flag, act, own, crossed, near, far):
    count = act.shape[0]
    hf = own.shape[1]
    return pl.pallas_call(
        down_kernel,
        out_shape=jax.ShapeDtypeStruct((count, D), jnp.bfloat16),
        in_specs=[pl.BlockSpec(memory_space=pltpu.SMEM), pl.BlockSpec(memory_space=pltpu.VMEM)]
        + [pl.BlockSpec(memory_space=pltpu.HBM)] * 4,
        out_specs=pl.BlockSpec(memory_space=pltpu.VMEM),
        scratch_shapes=[
            pltpu.VMEM((2 * hf, D), jnp.bfloat16),
            pltpu.SemaphoreType.DMA((2, OUT_STEPS)),
        ],
        compiler_params=pltpu.CompilerParams(vmem_limit_bytes=20 * 1024 * 1024),
        cost_estimate=pl.CostEstimate(
            flops=4 * count * D * hf, bytes_accessed=4 * D * hf + 2 * count * D, transcendentals=0
        ),
        name="expert_down",
    )(flag, act, own, crossed, near, far)


def local(
    resid,
    queries,
    new_keys,
    new_values,
    cache_keys,
    cache_values,
    cache_len,
    out_proj,
    norm_gain,
    router,
    expert_ids,
    gate_slab,
    up_slab,
    down_slab,
):
    rows = resid.shape[0]
    chips = lax.axis_size("chip")
    core = lax.axis_index("core")
    depth = lax.axis_index("dp")
    depths = lax.axis_size("dp")

    other_proj = flipped(out_proj, "core", 1)
    spots = [(c, d) for c in range(2) for d in range(depths)]
    across = [(c * depths + d, c * depths + (d ^ 1)) for c, d in spots if c != d % 2]
    beside = [(c * depths + d, (1 - c) * depths + d) for c, d in spots if c == d % 2]

    def moved(slab, pairs, after=None):
        if after is not None:
            slab, _ = lax.optimization_barrier((slab, after))
        return lax.ppermute(slab, ("core", "dp"), pairs)

    gate_crossed = moved(gate_slab, across)
    gate_near = moved(gate_slab, beside)
    up_near = moved(up_slab, beside)
    down_near = moved(down_slab, beside)
    flag = (core == depth % 2).astype(jnp.int32).reshape(1)
    ring = [(c * depths + d, c * depths + (d + 1 - 2 * c) % depths) for c, d in spots]

    def gathered(value):
        blocks = [value]
        for _ in range(depths - 1):
            blocks.append(lax.ppermute(blocks[-1], ("core", "dp"), ring))
        return blocks

    id_blocks = gathered(expert_ids)
    ids = jnp.concatenate(id_blocks, axis=0)

    piece = out_proj.shape[0]
    sent = attention(
        core.astype(jnp.int32).reshape(1),
        queries,
        new_keys,
        new_values,
        cache_keys,
        cache_values,
        cache_len,
        chips,
    )
    regrouped = lax.all_to_all(sent, "chip", split_axis=0, concat_axis=0, tiled=True)
    regrouped = regrouped.reshape(chips * rows, 2 * piece)
    partial = jnp.dot(regrouped[:, :piece], out_proj, preferred_element_type=jnp.float32)
    partial = partial + jnp.dot(
        regrouped[:, piece:], other_proj, preferred_element_type=jnp.float32
    )
    count = ids.shape[0]
    labels = 4 * jnp.arange(chips, dtype=jnp.int32) + 2 * (depth % 2) + depth // 2
    hits = ids.T[:, None, :] == labels[None, :, None]
    member = jnp.any(hits, axis=0)
    at = jnp.arange(count, dtype=jnp.int32)
    before = (at[:, None] < at[None, :]) & (at[:, None] // rows == at[None, :] // rows)
    rank = jnp.dot(
        member.astype(jnp.bfloat16),
        before.astype(jnp.bfloat16),
        preferred_element_type=jnp.float32,
    ).astype(jnp.int32)
    place = jnp.where(member, rank + CAP * (at // rows)[None, :], -1)
    slots = CAP * depths
    dispatch = place[:, None, :] == jnp.arange(slots, dtype=jnp.int32)[None, :, None]

    partial = partial.astype(jnp.bfloat16)
    up_crossed = moved(up_slab, across, partial)
    down_crossed = moved(down_slab, across, partial)
    partial = lax.all_to_all(
        partial.reshape(chips, rows, D),
        "chip",
        split_axis=0,
        concat_axis=0,
        tiled=True,
    )
    partial, dispatch = lax.optimization_barrier((partial, dispatch))
    hidden = resid.astype(jnp.float32) + jnp.sum(partial.astype(jnp.float32), axis=0)
    meansq = jnp.mean(hidden * hidden, axis=1, keepdims=True)
    normed = (hidden * lax.rsqrt(jnp.maximum(meansq, 0.25)) * norm_gain).astype(jnp.bfloat16)

    tokens = jnp.concatenate(gathered(normed), axis=0)
    outgoing = jnp.dot(
        dispatch.reshape(chips * slots, count).astype(jnp.bfloat16),
        tokens,
        preferred_element_type=jnp.float32,
    ).astype(jnp.bfloat16)
    gate_far = moved(gate_crossed, beside, outgoing)
    up_far = moved(up_crossed, beside, outgoing)
    down_far = moved(down_crossed, beside, outgoing)
    incoming = lax.all_to_all(
        outgoing.reshape(chips, slots, D), "chip", split_axis=0, concat_axis=0, tiled=True
    )

    logits = jnp.dot(tokens, router, preferred_element_type=jnp.float32)
    experts = router.shape[1]
    onehot = ids[:, :, None] == jnp.arange(experts, dtype=jnp.int32)[None, None, :]
    chosen = jnp.sum(jnp.where(onehot, logits[:, None, :], 0.0), axis=2)
    peak_logit = jnp.max(chosen, axis=1, keepdims=True)
    exp_logit = jnp.exp(chosen - peak_logit)
    gate_probs = (exp_logit / jnp.sum(exp_logit, axis=1, keepdims=True)).astype(jnp.bfloat16)
    spread = jnp.sum(
        jnp.where(hits, gate_probs.astype(jnp.float32).T[:, None, :], 0.0), axis=0
    )
    combine = jnp.where(dispatch, spread[:, None, :], 0.0).astype(jnp.bfloat16)

    act = expert_act(
        flag,
        incoming.reshape(chips * slots, D),
        (gate_slab, up_slab),
        (gate_crossed, up_crossed),
        (gate_near, up_near),
        (gate_far, up_far),
    )
    produced = expert_down(flag, act, down_slab, down_crossed, down_near, down_far)
    returned = lax.all_to_all(
        produced.reshape(chips, slots, D), "chip", split_axis=0, concat_axis=0, tiled=True
    )
    mix = lax.dot_general(
        combine.reshape(chips * slots, count),
        returned.reshape(chips * slots, D),
        (((0,), (0,)), ((), ())),
        preferred_element_type=jnp.float32,
    )
    total = hidden + mix[:rows]
    narrow = mix.astype(jnp.bfloat16)
    for m in range(1, depths):
        home = [(c * depths + d, c * depths + (d + (2 * c - 1) * m) % depths) for c, d in spots]
        part = lax.ppermute(narrow[m * rows : (m + 1) * rows], ("core", "dp"), home)
        total = total + part.astype(jnp.float32)
    return total


def solution(mesh):
    split = Mesh(mesh.devices.reshape(-1, 2, mesh.shape["dp"]), ALL)
    in_specs = (
        P(ALL, None),
        P(ALL, None),
        P(ALL, None),
        P(ALL, None),
        P(ALL, None, None),
        P(ALL, None, None),
        P(ALL),
        P(EP, None),
        P(),
        P(),
        P(ALL, None),
        P(ALL, None, None),
        P(ALL, None, None),
        P(ALL, None, None),
    )

    return jax.shard_map(
        local, mesh=split, in_specs=in_specs, out_specs=P(ALL, None), check_vma=False
    )
```

```python
import math

import jax
import jax.numpy as jnp
from jax import lax
from jax.experimental import pallas as pl
from jax.experimental.pallas import tpu as pltpu
from jax.sharding import Mesh
from jax.sharding import PartitionSpec as P

D = 4096
H = 64
KVH = 4
HD = 128
CAP = 4
ATTN_STEPS = 2
OUT_STEPS = 2
CUTS = 8
X_CUTS = 4


EP = ("chip", "core")
ALL = ("chip", "core", "dp")


def flipped(value, axis, mask):
    pairs = [(source, source ^ mask) for source in range(lax.axis_size(axis))]
    return lax.ppermute(value, axis, pairs)


def attention_kernel(swap, lengths, q_in, nk_in, nv_in, keys, values, out, q_buf, o_buf):
    step = pl.program_id(0)
    tokens = q_in.shape[0]
    group = H // KVH
    scale = 1.0 / math.sqrt(HD)

    @pl.when(step == 0)
    def _():
        for head in range(H):
            q_buf[pl.ds(head, tokens, stride=H), :] = q_in[:, head * HD : (head + 1) * HD].astype(
                jnp.float32
            )

    nk = nk_in[...].astype(jnp.float32)
    nv = nv_in[...].astype(jnp.float32)
    span = keys.shape[1]
    owner = lax.broadcasted_iota(jnp.int32, (H, HD), 0) // group
    position = lax.broadcasted_iota(jnp.int32, (H, span), 1)
    for local_row in range(keys.shape[0]):
        row = step * keys.shape[0] + local_row
        q = q_buf[pl.ds(row * H, H), :]
        blocks = [jnp.where(owner == g, q, 0.0).astype(jnp.bfloat16) for g in range(KVH)]
        scores = scale * lax.dot_general(
            jnp.concatenate(blocks, axis=1),
            keys[local_row],
            (((1,), (1,)), ((), ())),
            preferred_element_type=jnp.float32,
        )
        new_key = jnp.concatenate(
            [
                jnp.broadcast_to(nk[local_row : local_row + 1, g * HD : (g + 1) * HD], (group, HD))
                for g in range(KVH)
            ],
            axis=0,
        )
        new_value = jnp.concatenate(
            [
                jnp.broadcast_to(nv[local_row : local_row + 1, g * HD : (g + 1) * HD], (group, HD))
                for g in range(KVH)
            ],
            axis=0,
        )
        own = scale * jnp.sum(q * new_key, axis=1, keepdims=True)
        scores = jnp.where(position < lengths[row], scores, -1e30)
        peak = jnp.maximum(jnp.max(scores, axis=1, keepdims=True), own)
        past_exp = jnp.exp(scores - peak)
        own_exp = jnp.exp(own - peak)
        denom = jnp.sum(past_exp, axis=1, keepdims=True) + own_exp
        weights = (past_exp / denom).astype(jnp.bfloat16)
        own_weight = (own_exp / denom).astype(jnp.bfloat16).astype(jnp.float32)
        wide = jnp.dot(weights, values[local_row], preferred_element_type=jnp.float32)
        blended = jnp.concatenate(
            [wide[g * group : (g + 1) * group, g * HD : (g + 1) * HD] for g in range(KVH)], axis=0
        )
        o_buf[pl.ds(row * H, H), :] = blended + own_weight * new_value

    @pl.when(step == pl.num_programs(0) - 1)
    def _():
        chips, _, width = out.shape
        per = width // HD
        for chip in range(chips):
            for at in range(per):
                head = chip * per + at
                first = o_buf[pl.ds(head, tokens, stride=H), :]
                second = o_buf[pl.ds(chip * per + (at ^ (per // 2)), tokens, stride=H), :]
                out[chip, :, at * HD : (at + 1) * HD] = jnp.where(
                    swap[0] == 1, second, first
                ).astype(jnp.bfloat16)


def attention(swap, queries, new_keys, new_values, cache_keys, cache_values, cache_len, chips):
    rows = queries.shape[0]
    span = cache_keys.shape[1]
    each = rows // ATTN_STEPS
    smem = pl.BlockSpec(memory_space=pltpu.SMEM)
    return pl.pallas_call(
        attention_kernel,
        grid=(ATTN_STEPS,),
        out_shape=jax.ShapeDtypeStruct((chips, rows, H * HD // chips), jnp.bfloat16),
        in_specs=[
            smem,
            smem,
            pl.BlockSpec((rows, H * HD), lambda i: (0, 0)),
            pl.BlockSpec((each, KVH * HD), lambda i: (i, 0)),
            pl.BlockSpec((each, KVH * HD), lambda i: (i, 0)),
            pl.BlockSpec((each, span, KVH * HD), lambda i: (i, 0, 0)),
            pl.BlockSpec((each, span, KVH * HD), lambda i: (i, 0, 0)),
        ],
        out_specs=pl.BlockSpec((chips, rows, H * HD // chips), lambda i: (0, 0, 0)),
        scratch_shapes=[
            pltpu.VMEM((rows * H, HD), jnp.float32),
            pltpu.VMEM((rows * H, HD), jnp.float32),
        ],
        compiler_params=pltpu.CompilerParams(dimension_semantics=("arbitrary",)),
        cost_estimate=pl.CostEstimate(
            flops=8 * rows * H * HD * span, bytes_accessed=4 * rows * span * KVH * HD, transcendentals=0
        ),
        name="attention",
    )(swap, cache_len, queries, new_keys, new_values, cache_keys, cache_values)


def ffn_kernel(flag, rows_in, *refs):
    own, crossed, near, far = refs[0:3], refs[3:6], refs[6:9], refs[9:12]
    out, x_buf, in_buf, down_buf, y_buf, x_sem, in_sem, down_sem, y_sem = refs[12:]
    hf = own[0].shape[2]
    deep = D // CUTS
    wide = D // OUT_STEPS

    def x_copy(cut):
        part = pl.ds(cut * rows_in.shape[0] // X_CUTS, rows_in.shape[0] // X_CUTS)
        return pltpu.make_async_copy(rows_in.at[part], x_buf.at[part], x_sem.at[cut])

    def in_copy(side, source, part, cut):
        return pltpu.make_async_copy(
            source[part].at[0, pl.ds(cut * deep, deep)],
            in_buf.at[2 * side + part, pl.ds(cut * deep, deep)],
            in_sem.at[2 * side + part, cut],
        )

    def down_copy(side, source, step):
        return pltpu.make_async_copy(
            source[2].at[0, :, pl.ds(step * wide, wide)],
            down_buf.at[pl.ds(side * hf, hf), pl.ds(step * wide, wide)],
            down_sem.at[side, step],
        )

    def start(first, second):
        for side, source in ((0, first), (1, second)):
            for part in range(2):
                for cut in range(CUTS):
                    in_copy(side, source, part, cut).start()
        for step in range(OUT_STEPS):
            down_copy(0, first, step).start()
            down_copy(1, second, step).start()

    for cut in range(X_CUTS):
        x_copy(cut).start()

    @pl.when(flag[0] == 1)
    def _():
        start(own, crossed)

    @pl.when(flag[0] != 1)
    def _():
        start(near, far)

    for cut in range(X_CUTS):
        x_copy(cut).wait()
    acts = []
    for side in range(2):
        vals = []
        for part in range(2):
            for cut in range(CUTS):
                in_copy(side, own, part, cut).wait()
            vals.append(
                jnp.dot(x_buf[...], in_buf[2 * side + part], preferred_element_type=jnp.float32)
            )
        gate_val, up_val = vals
        acts.append((gate_val / (1.0 + jnp.exp(-gate_val)) * up_val).astype(jnp.bfloat16))
    act = jnp.concatenate(acts, axis=1)
    copies = []
    for step in range(OUT_STEPS):
        columns = slice(step * wide, (step + 1) * wide)
        for side in range(2):
            down_copy(side, own, step).wait()
        y_buf[:, columns] = jnp.dot(
            act, down_buf[:, columns], preferred_element_type=jnp.float32
        ).astype(jnp.bfloat16)
        copy = pltpu.make_async_copy(
            y_buf.at[:, pl.ds(step * wide, wide)],
            out.at[:, pl.ds(step * wide, wide)],
            y_sem.at[step],
        )
        copy.start()
        copies.append(copy)
    for copy in copies:
        copy.wait()


def expert_ffn(flag, rows_in, own, crossed, near, far):
    count = rows_in.shape[0]
    hf = own[0].shape[2]
    return pl.pallas_call(
        ffn_kernel,
        out_shape=jax.ShapeDtypeStruct((count, D), jnp.bfloat16),
        in_specs=[pl.BlockSpec(memory_space=pltpu.SMEM)]
        + [pl.BlockSpec(memory_space=pltpu.HBM)] * 13,
        out_specs=pl.BlockSpec(memory_space=pltpu.HBM),
        scratch_shapes=[
            pltpu.VMEM((count, D), jnp.bfloat16),
            pltpu.VMEM((4, D, hf), jnp.bfloat16),
            pltpu.VMEM((2 * hf, D), jnp.bfloat16),
            pltpu.VMEM((count, D), jnp.bfloat16),
            pltpu.SemaphoreType.DMA((X_CUTS,)),
            pltpu.SemaphoreType.DMA((4, CUTS)),
            pltpu.SemaphoreType.DMA((2, OUT_STEPS)),
            pltpu.SemaphoreType.DMA((OUT_STEPS,)),
        ],
        compiler_params=pltpu.CompilerParams(vmem_limit_bytes=123 * 512 * 1024),
        cost_estimate=pl.CostEstimate(
            flops=12 * count * D * hf, bytes_accessed=12 * D * hf + 4 * count * D, transcendentals=0
        ),
        name="expert_ffn",
    )(flag, rows_in, *own, *crossed, *near, *far)


def local(
    resid,
    queries,
    new_keys,
    new_values,
    cache_keys,
    cache_values,
    cache_len,
    out_proj,
    norm_gain,
    router,
    expert_ids,
    gate_slab,
    up_slab,
    down_slab,
):
    rows = resid.shape[0]
    chips = lax.axis_size("chip")
    core = lax.axis_index("core")
    depth = lax.axis_index("dp")
    depths = lax.axis_size("dp")

    other_proj = flipped(out_proj, "core", 1)
    spots = [(c, d) for c in range(2) for d in range(depths)]
    across = [(c * depths + d, c * depths + (d ^ 1)) for c, d in spots if c != d % 2]
    beside = [(c * depths + d, (1 - c) * depths + d) for c, d in spots if c == d % 2]

    def moved(slab, pairs, after=None):
        if after is not None:
            slab, _ = lax.optimization_barrier((slab, after))
        return lax.ppermute(slab, ("core", "dp"), pairs)

    gate_crossed = moved(gate_slab, across)
    gate_near = moved(gate_slab, beside)
    up_near = moved(up_slab, beside)
    down_near = moved(down_slab, beside)
    flag = (core == depth % 2).astype(jnp.int32).reshape(1)
    ring = [(c * depths + d, c * depths + (d + 1 - 2 * c) % depths) for c, d in spots]

    def gathered(value):
        blocks = [value]
        for _ in range(depths - 1):
            blocks.append(lax.ppermute(blocks[-1], ("core", "dp"), ring))
        return blocks

    id_blocks = gathered(expert_ids)
    ids = jnp.concatenate(id_blocks, axis=0)

    piece = out_proj.shape[0]
    sent = attention(
        core.astype(jnp.int32).reshape(1),
        queries,
        new_keys,
        new_values,
        cache_keys,
        cache_values,
        cache_len,
        chips,
    )
    regrouped = lax.all_to_all(sent, "chip", split_axis=0, concat_axis=0, tiled=True)
    regrouped = regrouped.reshape(chips * rows, 2 * piece)
    partial = jnp.dot(regrouped[:, :piece], out_proj, preferred_element_type=jnp.float32)
    partial = partial + jnp.dot(
        regrouped[:, piece:], other_proj, preferred_element_type=jnp.float32
    )
    count = ids.shape[0]
    labels = 4 * jnp.arange(chips, dtype=jnp.int32) + 2 * (depth % 2) + depth // 2
    hits = ids.T[:, None, :] == labels[None, :, None]
    member = jnp.any(hits, axis=0)
    at = jnp.arange(count, dtype=jnp.int32)
    before = (at[:, None] < at[None, :]) & (at[:, None] // rows == at[None, :] // rows)
    rank = jnp.dot(
        member.astype(jnp.bfloat16),
        before.astype(jnp.bfloat16),
        preferred_element_type=jnp.float32,
    ).astype(jnp.int32)
    place = jnp.where(member, rank + CAP * (at // rows)[None, :], -1)
    slots = CAP * depths
    dispatch = place[:, None, :] == jnp.arange(slots, dtype=jnp.int32)[None, :, None]

    partial = partial.astype(jnp.bfloat16)
    up_crossed = moved(up_slab, across, partial)
    down_crossed = moved(down_slab, across, partial)
    partial = lax.all_to_all(
        partial.reshape(chips, rows, D),
        "chip",
        split_axis=0,
        concat_axis=0,
        tiled=True,
    )
    partial, dispatch = lax.optimization_barrier((partial, dispatch))
    hidden = resid.astype(jnp.float32) + jnp.sum(partial.astype(jnp.float32), axis=0)
    meansq = jnp.mean(hidden * hidden, axis=1, keepdims=True)
    normed = (hidden * lax.rsqrt(jnp.maximum(meansq, 0.25)) * norm_gain).astype(jnp.bfloat16)

    tokens = jnp.concatenate(gathered(normed), axis=0)
    outgoing = jnp.dot(
        dispatch.reshape(chips * slots, count).astype(jnp.bfloat16),
        tokens,
        preferred_element_type=jnp.float32,
    ).astype(jnp.bfloat16)
    gate_far = moved(gate_crossed, beside, outgoing)
    up_far = moved(up_crossed, beside, outgoing)
    down_far = moved(down_crossed, beside, outgoing)
    incoming = lax.all_to_all(
        outgoing.reshape(chips, slots, D), "chip", split_axis=0, concat_axis=0, tiled=True
    )

    logits = jnp.dot(tokens, router, preferred_element_type=jnp.float32)
    experts = router.shape[1]
    onehot = ids[:, :, None] == jnp.arange(experts, dtype=jnp.int32)[None, None, :]
    chosen = jnp.sum(jnp.where(onehot, logits[:, None, :], 0.0), axis=2)
    peak_logit = jnp.max(chosen, axis=1, keepdims=True)
    exp_logit = jnp.exp(chosen - peak_logit)
    gate_probs = (exp_logit / jnp.sum(exp_logit, axis=1, keepdims=True)).astype(jnp.bfloat16)
    spread = jnp.sum(
        jnp.where(hits, gate_probs.astype(jnp.float32).T[:, None, :], 0.0), axis=0
    )
    combine = jnp.where(dispatch, spread[:, None, :], 0.0).astype(jnp.bfloat16)

    produced = expert_ffn(
        flag,
        incoming.reshape(chips * slots, D),
        (gate_slab, up_slab, down_slab),
        (gate_crossed, up_crossed, down_crossed),
        (gate_near, up_near, down_near),
        (gate_far, up_far, down_far),
    )
    returned = lax.all_to_all(
        produced.reshape(chips, slots, D), "chip", split_axis=0, concat_axis=0, tiled=True
    )
    mix = lax.dot_general(
        combine.reshape(chips * slots, count),
        returned.reshape(chips * slots, D),
        (((0,), (0,)), ((), ())),
        preferred_element_type=jnp.float32,
    )
    total = hidden + mix[:rows]
    narrow = mix.astype(jnp.bfloat16)
    for m in range(1, depths):
        home = [(c * depths + d, c * depths + (d + (2 * c - 1) * m) % depths) for c, d in spots]
        part = lax.ppermute(narrow[m * rows : (m + 1) * rows], ("core", "dp"), home)
        total = total + part.astype(jnp.float32)
    return total


def solution(mesh):
    split = Mesh(mesh.devices.reshape(-1, 2, mesh.shape["dp"]), ALL)
    in_specs = (
        P(ALL, None),
        P(ALL, None),
        P(ALL, None),
        P(ALL, None),
        P(ALL, None, None),
        P(ALL, None, None),
        P(ALL),
        P(EP, None),
        P(),
        P(),
        P(ALL, None),
        P(ALL, None, None),
        P(ALL, None, None),
        P(ALL, None, None),
    )

    return jax.shard_map(
        local, mesh=split, in_specs=in_specs, out_specs=P(ALL, None), check_vma=False
    )
```

```python
import math

import jax
import jax.numpy as jnp
from jax import lax
from jax.experimental import pallas as pl
from jax.experimental.pallas import tpu as pltpu
from jax.sharding import Mesh
from jax.sharding import PartitionSpec as P

D = 4096
H = 64
KVH = 4
HD = 128
CAP = 4
ATTN_STEPS = 2
OUT_STEPS = 2
CUTS = 8
X_CUTS = 4
COMBINE_STEPS = 4


EP = ("chip", "core")
ALL = ("chip", "core", "dp")


def flipped(value, axis, mask):
    pairs = [(source, source ^ mask) for source in range(lax.axis_size(axis))]
    return lax.ppermute(value, axis, pairs)


def attention_kernel(swap, lengths, q_in, nk_in, nv_in, keys, values, out, q_buf, o_buf):
    step = pl.program_id(0)
    tokens = q_in.shape[0]
    group = H // KVH
    scale = 1.0 / math.sqrt(HD)

    @pl.when(step == 0)
    def _():
        for head in range(H):
            q_buf[pl.ds(head, tokens, stride=H), :] = q_in[:, head * HD : (head + 1) * HD].astype(
                jnp.float32
            )

    nk = nk_in[...].astype(jnp.float32)
    nv = nv_in[...].astype(jnp.float32)
    span = keys.shape[1]
    owner = lax.broadcasted_iota(jnp.int32, (H, HD), 0) // group
    position = lax.broadcasted_iota(jnp.int32, (H, span), 1)
    for local_row in range(keys.shape[0]):
        row = step * keys.shape[0] + local_row
        q = q_buf[pl.ds(row * H, H), :]
        blocks = [jnp.where(owner == g, q, 0.0).astype(jnp.bfloat16) for g in range(KVH)]
        scores = scale * lax.dot_general(
            jnp.concatenate(blocks, axis=1),
            keys[local_row],
            (((1,), (1,)), ((), ())),
            preferred_element_type=jnp.float32,
        )
        new_key = jnp.concatenate(
            [
                jnp.broadcast_to(nk[local_row : local_row + 1, g * HD : (g + 1) * HD], (group, HD))
                for g in range(KVH)
            ],
            axis=0,
        )
        new_value = jnp.concatenate(
            [
                jnp.broadcast_to(nv[local_row : local_row + 1, g * HD : (g + 1) * HD], (group, HD))
                for g in range(KVH)
            ],
            axis=0,
        )
        own = scale * jnp.sum(q * new_key, axis=1, keepdims=True)
        scores = jnp.where(position < lengths[row], scores, -1e30)
        peak = jnp.maximum(jnp.max(scores, axis=1, keepdims=True), own)
        past_exp = jnp.exp(scores - peak)
        own_exp = jnp.exp(own - peak)
        denom = jnp.sum(past_exp, axis=1, keepdims=True) + own_exp
        weights = (past_exp / denom).astype(jnp.bfloat16)
        own_weight = (own_exp / denom).astype(jnp.bfloat16).astype(jnp.float32)
        wide = jnp.dot(weights, values[local_row], preferred_element_type=jnp.float32)
        blended = jnp.concatenate(
            [wide[g * group : (g + 1) * group, g * HD : (g + 1) * HD] for g in range(KVH)], axis=0
        )
        o_buf[pl.ds(row * H, H), :] = blended + own_weight * new_value

    @pl.when(step == pl.num_programs(0) - 1)
    def _():
        chips, _, width = out.shape
        per = width // HD
        for chip in range(chips):
            for at in range(per):
                head = chip * per + at
                first = o_buf[pl.ds(head, tokens, stride=H), :]
                second = o_buf[pl.ds(chip * per + (at ^ (per // 2)), tokens, stride=H), :]
                out[chip, :, at * HD : (at + 1) * HD] = jnp.where(
                    swap[0] == 1, second, first
                ).astype(jnp.bfloat16)


def attention(swap, queries, new_keys, new_values, cache_keys, cache_values, cache_len, chips):
    rows = queries.shape[0]
    span = cache_keys.shape[1]
    each = rows // ATTN_STEPS
    smem = pl.BlockSpec(memory_space=pltpu.SMEM)
    return pl.pallas_call(
        attention_kernel,
        grid=(ATTN_STEPS,),
        out_shape=jax.ShapeDtypeStruct((chips, rows, H * HD // chips), jnp.bfloat16),
        in_specs=[
            smem,
            smem,
            pl.BlockSpec((rows, H * HD), lambda i: (0, 0)),
            pl.BlockSpec((each, KVH * HD), lambda i: (i, 0)),
            pl.BlockSpec((each, KVH * HD), lambda i: (i, 0)),
            pl.BlockSpec((each, span, KVH * HD), lambda i: (i, 0, 0)),
            pl.BlockSpec((each, span, KVH * HD), lambda i: (i, 0, 0)),
        ],
        out_specs=pl.BlockSpec((chips, rows, H * HD // chips), lambda i: (0, 0, 0)),
        scratch_shapes=[
            pltpu.VMEM((rows * H, HD), jnp.float32),
            pltpu.VMEM((rows * H, HD), jnp.float32),
        ],
        compiler_params=pltpu.CompilerParams(dimension_semantics=("arbitrary",)),
        cost_estimate=pl.CostEstimate(
            flops=8 * rows * H * HD * span, bytes_accessed=4 * rows * span * KVH * HD, transcendentals=0
        ),
        name="attention",
    )(swap, cache_len, queries, new_keys, new_values, cache_keys, cache_values)


def ffn_kernel(flag, rows_in, *refs):
    own, crossed, near, far = refs[0:3], refs[3:6], refs[6:9], refs[9:12]
    out, x_buf, in_buf, down_buf, y_buf, x_sem, in_sem, down_sem, y_sem = refs[12:]
    hf = own[0].shape[2]
    deep = D // CUTS
    wide = D // OUT_STEPS

    def x_copy(cut):
        part = pl.ds(cut * rows_in.shape[0] // X_CUTS, rows_in.shape[0] // X_CUTS)
        return pltpu.make_async_copy(rows_in.at[part], x_buf.at[part], x_sem.at[cut])

    def in_copy(side, source, part, cut):
        return pltpu.make_async_copy(
            source[part].at[0, pl.ds(cut * deep, deep)],
            in_buf.at[2 * side + part, pl.ds(cut * deep, deep)],
            in_sem.at[2 * side + part, cut],
        )

    def down_copy(side, source, step):
        return pltpu.make_async_copy(
            source[2].at[0, :, pl.ds(step * wide, wide)],
            down_buf.at[pl.ds(side * hf, hf), pl.ds(step * wide, wide)],
            down_sem.at[side, step],
        )

    def start(first, second):
        for side, source in ((0, first), (1, second)):
            for part in range(2):
                for cut in range(CUTS):
                    in_copy(side, source, part, cut).start()
        for step in range(OUT_STEPS):
            down_copy(0, first, step).start()
            down_copy(1, second, step).start()

    for cut in range(X_CUTS):
        x_copy(cut).start()

    @pl.when(flag[0] == 1)
    def _():
        start(own, crossed)

    @pl.when(flag[0] != 1)
    def _():
        start(near, far)

    for cut in range(X_CUTS):
        x_copy(cut).wait()
    acts = []
    for side in range(2):
        vals = []
        for part in range(2):
            for cut in range(CUTS):
                in_copy(side, own, part, cut).wait()
            vals.append(
                jnp.dot(x_buf[...], in_buf[2 * side + part], preferred_element_type=jnp.float32)
            )
        gate_val, up_val = vals
        acts.append((gate_val / (1.0 + jnp.exp(-gate_val)) * up_val).astype(jnp.bfloat16))
    act = jnp.concatenate(acts, axis=1)
    copies = []
    for step in range(OUT_STEPS):
        columns = slice(step * wide, (step + 1) * wide)
        for side in range(2):
            down_copy(side, own, step).wait()
        rows_out = jnp.dot(act, down_buf[:, columns], preferred_element_type=jnp.float32)
        for chunk in range(out.shape[0]):
            y_buf[chunk, :, columns] = rows_out[chunk * CAP : (chunk + 1) * CAP].astype(
                jnp.bfloat16
            )
        copy = pltpu.make_async_copy(
            y_buf.at[:, :, pl.ds(step * wide, wide)],
            out.at[:, :, pl.ds(step * wide, wide)],
            y_sem.at[step],
        )
        copy.start()
        copies.append(copy)
    for copy in copies:
        copy.wait()


def expert_ffn(flag, rows_in, own, crossed, near, far):
    count = rows_in.shape[0]
    hf = own[0].shape[2]
    return pl.pallas_call(
        ffn_kernel,
        out_shape=jax.ShapeDtypeStruct((count // CAP, CAP, D), jnp.bfloat16),
        in_specs=[pl.BlockSpec(memory_space=pltpu.SMEM)]
        + [pl.BlockSpec(memory_space=pltpu.HBM)] * 13,
        out_specs=pl.BlockSpec(memory_space=pltpu.HBM),
        scratch_shapes=[
            pltpu.VMEM((count, D), jnp.bfloat16),
            pltpu.VMEM((4, D, hf), jnp.bfloat16),
            pltpu.VMEM((2 * hf, D), jnp.bfloat16),
            pltpu.VMEM((count // CAP, CAP, D), jnp.bfloat16),
            pltpu.SemaphoreType.DMA((X_CUTS,)),
            pltpu.SemaphoreType.DMA((4, CUTS)),
            pltpu.SemaphoreType.DMA((2, OUT_STEPS)),
            pltpu.SemaphoreType.DMA((OUT_STEPS,)),
        ],
        compiler_params=pltpu.CompilerParams(vmem_limit_bytes=123 * 512 * 1024),
        cost_estimate=pl.CostEstimate(
            flops=12 * count * D * hf, bytes_accessed=12 * D * hf + 4 * count * D, transcendentals=0
        ),
        name="expert_ffn",
    )(flag, rows_in, *own, *crossed, *near, *far)


def combine_kernel(weights, rows_in, hidden, out):
    flat = jnp.concatenate([rows_in[chunk] for chunk in range(rows_in.shape[0])], axis=0)
    out[...] = hidden[...] + jnp.dot(weights[...], flat, preferred_element_type=jnp.float32)


def combined(weights, rows_in, hidden):
    chunks, each, _ = rows_in.shape
    rows = hidden.shape[0]
    wide = D // COMBINE_STEPS
    return pl.pallas_call(
        combine_kernel,
        grid=(COMBINE_STEPS,),
        out_shape=jax.ShapeDtypeStruct((rows, D), jnp.float32),
        in_specs=[
            pl.BlockSpec((rows, chunks * each), lambda i: (0, 0)),
            pl.BlockSpec((chunks, each, wide), lambda i: (0, 0, i)),
            pl.BlockSpec((rows, wide), lambda i: (0, i)),
        ],
        out_specs=pl.BlockSpec((rows, wide), lambda i: (0, i)),
        compiler_params=pltpu.CompilerParams(
            dimension_semantics=("arbitrary",), vmem_limit_bytes=123 * 512 * 1024
        ),
        cost_estimate=pl.CostEstimate(
            flops=2 * rows * chunks * each * D, bytes_accessed=2 * chunks * each * D, transcendentals=0
        ),
        name="combined",
    )(weights, rows_in, hidden)


def local(
    resid,
    queries,
    new_keys,
    new_values,
    cache_keys,
    cache_values,
    cache_len,
    out_proj,
    norm_gain,
    router,
    expert_ids,
    gate_slab,
    up_slab,
    down_slab,
):
    rows = resid.shape[0]
    chips = lax.axis_size("chip")
    core = lax.axis_index("core")
    depth = lax.axis_index("dp")
    depths = lax.axis_size("dp")

    other_proj = flipped(out_proj, "core", 1)
    spots = [(c, d) for c in range(2) for d in range(depths)]
    across = [(c * depths + d, c * depths + (d ^ 1)) for c, d in spots if c != d % 2]
    beside = [(c * depths + d, (1 - c) * depths + d) for c, d in spots if c == d % 2]

    def moved(slab, pairs, after=None):
        if after is not None:
            slab, _ = lax.optimization_barrier((slab, after))
        return lax.ppermute(slab, ("core", "dp"), pairs)

    gate_crossed = moved(gate_slab, across)
    gate_near = moved(gate_slab, beside)
    up_near = moved(up_slab, beside)
    down_near = moved(down_slab, beside)
    flag = (core == depth % 2).astype(jnp.int32).reshape(1)
    ring = [(c * depths + d, c * depths + (d + 1 - 2 * c) % depths) for c, d in spots]

    def gathered(value):
        blocks = [value]
        for _ in range(depths - 1):
            blocks.append(lax.ppermute(blocks[-1], ("core", "dp"), ring))
        return blocks

    id_blocks = gathered(expert_ids)
    ids = jnp.concatenate(id_blocks, axis=0)

    piece = out_proj.shape[0]
    sent = attention(
        core.astype(jnp.int32).reshape(1),
        queries,
        new_keys,
        new_values,
        cache_keys,
        cache_values,
        cache_len,
        chips,
    )
    regrouped = lax.all_to_all(sent, "chip", split_axis=0, concat_axis=0, tiled=True)
    regrouped = regrouped.reshape(chips * rows, 2 * piece)
    partial = jnp.dot(regrouped[:, :piece], out_proj, preferred_element_type=jnp.float32)
    partial = partial + jnp.dot(
        regrouped[:, piece:], other_proj, preferred_element_type=jnp.float32
    )
    count = ids.shape[0]
    labels = 4 * jnp.arange(chips, dtype=jnp.int32) + 2 * (depth % 2) + depth // 2
    hits = ids.T[:, None, :] == labels[None, :, None]
    member = jnp.any(hits, axis=0)
    at = jnp.arange(count, dtype=jnp.int32)
    before = (at[:, None] < at[None, :]) & (at[:, None] // rows == at[None, :] // rows)
    rank = jnp.dot(
        member.astype(jnp.bfloat16),
        before.astype(jnp.bfloat16),
        preferred_element_type=jnp.float32,
    ).astype(jnp.int32)
    source = (depth + depths + (2 * core - 1) * (at // rows)) % depths
    place = jnp.where(member, rank + CAP * source[None, :], -1)
    slots = CAP * depths
    dispatch = place[:, None, :] == jnp.arange(slots, dtype=jnp.int32)[None, :, None]

    chunk = jnp.arange(chips * depths, dtype=jnp.int32)
    homes = 4 * (chunk // depths) + 2 * (chunk % 2) + (chunk % depths) // 2
    own_hits = expert_ids[:, :, None] == homes[None, None, :]
    own_member = jnp.any(own_hits, axis=1)
    turn = jnp.arange(rows, dtype=jnp.int32)
    own_rank = jnp.dot(
        (turn[None, :] < turn[:, None]).astype(jnp.bfloat16),
        own_member.astype(jnp.bfloat16),
        preferred_element_type=jnp.float32,
    ).astype(jnp.int32)
    own_rank = jnp.where(own_member, own_rank, -1)
    own_slots = own_rank[:, :, None] == jnp.arange(CAP, dtype=jnp.int32)[None, None, :]

    partial = partial.astype(jnp.bfloat16)
    up_crossed = moved(up_slab, across, partial)
    down_crossed = moved(down_slab, across, partial)
    partial = lax.all_to_all(
        partial.reshape(chips, rows, D),
        "chip",
        split_axis=0,
        concat_axis=0,
        tiled=True,
    )
    partial, dispatch, own_slots = lax.optimization_barrier((partial, dispatch, own_slots))
    hidden = resid.astype(jnp.float32) + jnp.sum(partial.astype(jnp.float32), axis=0)
    meansq = jnp.mean(hidden * hidden, axis=1, keepdims=True)
    normed = (hidden * lax.rsqrt(jnp.maximum(meansq, 0.25)) * norm_gain).astype(jnp.bfloat16)

    tokens = jnp.concatenate(gathered(normed), axis=0)
    outgoing = jnp.dot(
        dispatch.reshape(chips * slots, count).astype(jnp.bfloat16),
        tokens,
        preferred_element_type=jnp.float32,
    ).astype(jnp.bfloat16)
    gate_far = moved(gate_crossed, beside, outgoing)
    up_far = moved(up_crossed, beside, outgoing)
    down_far = moved(down_crossed, beside, outgoing)
    incoming = lax.all_to_all(
        outgoing.reshape(chips, slots, D), "chip", split_axis=0, concat_axis=0, tiled=True
    )

    logits = jnp.dot(normed, router, preferred_element_type=jnp.float32)
    experts = router.shape[1]
    onehot = expert_ids[:, :, None] == jnp.arange(experts, dtype=jnp.int32)[None, None, :]
    chosen = jnp.sum(jnp.where(onehot, logits[:, None, :], 0.0), axis=2)
    peak_logit = jnp.max(chosen, axis=1, keepdims=True)
    exp_logit = jnp.exp(chosen - peak_logit)
    gate_probs = (exp_logit / jnp.sum(exp_logit, axis=1, keepdims=True)).astype(jnp.bfloat16)
    spread = jnp.sum(jnp.where(own_hits, gate_probs.astype(jnp.float32)[:, :, None], 0.0), axis=1)
    combine = jnp.where(own_slots, spread[:, :, None], 0.0).astype(jnp.bfloat16)

    produced = expert_ffn(
        flag,
        incoming.reshape(chips * slots, D),
        (gate_slab, up_slab, down_slab),
        (gate_crossed, up_crossed, down_crossed),
        (gate_near, up_near, down_near),
        (gate_far, up_far, down_far),
    )
    returned = lax.all_to_all(produced, ("chip", "dp"), split_axis=0, concat_axis=0, tiled=True)
    return combined(combine.reshape(rows, chips * depths * CAP), returned, hidden)


def solution(mesh):
    split = Mesh(mesh.devices.reshape(-1, 2, mesh.shape["dp"]), ALL)
    in_specs = (
        P(ALL, None),
        P(ALL, None),
        P(ALL, None),
        P(ALL, None),
        P(ALL, None, None),
        P(ALL, None, None),
        P(ALL),
        P(EP, None),
        P(),
        P(),
        P(ALL, None),
        P(ALL, None, None),
        P(ALL, None, None),
        P(ALL, None, None),
    )

    return jax.shard_map(
        local, mesh=split, in_specs=in_specs, out_specs=P(ALL, None), check_vma=False
    )
```

```python
import math

import jax
import jax.numpy as jnp
from jax import lax
from jax.experimental import pallas as pl
from jax.experimental.pallas import tpu as pltpu
from jax.sharding import Mesh
from jax.sharding import PartitionSpec as P

D = 4096
H = 64
KVH = 4
HD = 128
CAP = 4
ATTN_STEPS = 2
OUT_STEPS = 2
CUTS = 8
X_CUTS = 4
COMBINE_STEPS = 2


EP = ("chip", "core")
ALL = ("chip", "core", "dp")


def flipped(value, axis, mask):
    pairs = [(source, source ^ mask) for source in range(lax.axis_size(axis))]
    return lax.ppermute(value, axis, pairs)


def attention_kernel(swap, lengths, q_in, nk_in, nv_in, keys, values, out, q_buf, o_buf):
    step = pl.program_id(0)
    tokens = q_in.shape[0]
    group = H // KVH
    scale = 1.0 / math.sqrt(HD)

    @pl.when(step == 0)
    def _():
        for head in range(H):
            q_buf[pl.ds(head, tokens, stride=H), :] = q_in[:, head * HD : (head + 1) * HD].astype(
                jnp.float32
            )

    nk = nk_in[...].astype(jnp.float32)
    nv = nv_in[...].astype(jnp.float32)
    span = keys.shape[1]
    owner = lax.broadcasted_iota(jnp.int32, (H, HD), 0) // group
    position = lax.broadcasted_iota(jnp.int32, (H, span), 1)
    each = keys.shape[0]
    base = step * each
    q_all = q_buf[pl.ds(base * H, each * H), :]

    def fanned(value):
        return jnp.concatenate(
            [
                jnp.broadcast_to(value[row : row + 1, g * HD : (g + 1) * HD], (group, HD))
                for row in range(each)
                for g in range(KVH)
            ],
            axis=0,
        )

    past = []
    for row in range(each):
        q = q_all[row * H : (row + 1) * H]
        blocks = [jnp.where(owner == g, q, 0.0).astype(jnp.bfloat16) for g in range(KVH)]
        scores = scale * lax.dot_general(
            jnp.concatenate(blocks, axis=1),
            keys[row],
            (((1,), (1,)), ((), ())),
            preferred_element_type=jnp.float32,
        )
        past.append(jnp.where(position < lengths[base + row], scores, -1e30))
    past = jnp.concatenate(past, axis=0)
    own = scale * jnp.sum(q_all * fanned(nk), axis=1, keepdims=True)
    peak = jnp.maximum(jnp.max(past, axis=1, keepdims=True), own)
    past_exp = jnp.exp(past - peak)
    own_exp = jnp.exp(own - peak)
    denom = jnp.sum(past_exp, axis=1, keepdims=True) + own_exp
    weights = (past_exp / denom).astype(jnp.bfloat16)
    own_part = (own_exp / denom).astype(jnp.bfloat16).astype(jnp.float32) * fanned(nv)
    for row in range(each):
        wide = jnp.dot(
            weights[row * H : (row + 1) * H], values[row], preferred_element_type=jnp.float32
        )
        blended = jnp.concatenate(
            [wide[g * group : (g + 1) * group, g * HD : (g + 1) * HD] for g in range(KVH)], axis=0
        )
        o_buf[pl.ds((base + row) * H, H), :] = blended + own_part[row * H : (row + 1) * H]

    @pl.when(step == pl.num_programs(0) - 1)
    def _():
        chips, _, width = out.shape
        per = width // HD
        for chip in range(chips):
            for at in range(per):
                head = chip * per + at
                first = o_buf[pl.ds(head, tokens, stride=H), :]
                second = o_buf[pl.ds(chip * per + (at ^ (per // 2)), tokens, stride=H), :]
                out[chip, :, at * HD : (at + 1) * HD] = jnp.where(
                    swap[0] == 1, second, first
                ).astype(jnp.bfloat16)


def attention(swap, queries, new_keys, new_values, cache_keys, cache_values, cache_len, chips):
    rows = queries.shape[0]
    span = cache_keys.shape[1]
    each = rows // ATTN_STEPS
    smem = pl.BlockSpec(memory_space=pltpu.SMEM)
    return pl.pallas_call(
        attention_kernel,
        grid=(ATTN_STEPS,),
        out_shape=jax.ShapeDtypeStruct((chips, rows, H * HD // chips), jnp.bfloat16),
        in_specs=[
            smem,
            smem,
            pl.BlockSpec((rows, H * HD), lambda i: (0, 0)),
            pl.BlockSpec((each, KVH * HD), lambda i: (i, 0)),
            pl.BlockSpec((each, KVH * HD), lambda i: (i, 0)),
            pl.BlockSpec((each, span, KVH * HD), lambda i: (i, 0, 0)),
            pl.BlockSpec((each, span, KVH * HD), lambda i: (i, 0, 0)),
        ],
        out_specs=pl.BlockSpec((chips, rows, H * HD // chips), lambda i: (0, 0, 0)),
        scratch_shapes=[
            pltpu.VMEM((rows * H, HD), jnp.float32),
            pltpu.VMEM((rows * H, HD), jnp.float32),
        ],
        compiler_params=pltpu.CompilerParams(dimension_semantics=("arbitrary",)),
        cost_estimate=pl.CostEstimate(
            flops=8 * rows * H * HD * span, bytes_accessed=4 * rows * span * KVH * HD, transcendentals=0
        ),
        name="attention",
    )(swap, cache_len, queries, new_keys, new_values, cache_keys, cache_values)


def ffn_kernel(flag, rows_in, *refs):
    own, crossed, near, far = refs[0:3], refs[3:7], refs[7:10], refs[10:14]
    out, x_buf, in_buf, down_buf, y_buf, x_sem, in_sem, down_sem, y_sem = refs[14:]
    hf = own[0].shape[2]
    deep = D // CUTS
    wide = D // OUT_STEPS

    def x_copy(cut):
        part = pl.ds(cut * rows_in.shape[0] // X_CUTS, rows_in.shape[0] // X_CUTS)
        return pltpu.make_async_copy(rows_in.at[part], x_buf.at[part], x_sem.at[cut])

    def in_copy(side, source, part, cut):
        return pltpu.make_async_copy(
            source[part].at[0, pl.ds(cut * deep, deep)],
            in_buf.at[2 * side + part, pl.ds(cut * deep, deep)],
            in_sem.at[2 * side + part, cut],
        )

    def down_copy(row, source, step):
        return pltpu.make_async_copy(
            source.at[0, :, pl.ds(step * wide, wide)],
            down_buf.at[pl.ds(row, source.shape[1]), pl.ds(step * wide, wide)],
            down_sem.at[row // (hf // 2), step],
        )

    def down_copies(first, second, step):
        return (
            down_copy(0, first[2], step),
            down_copy(hf, second[2], step),
            down_copy(hf + hf // 2, second[3], step),
        )

    def start(first, second):
        for side, source in ((0, first), (1, second)):
            for part in range(2):
                for cut in range(CUTS):
                    in_copy(side, source, part, cut).start()
        for step in range(OUT_STEPS):
            for copy in down_copies(first, second, step):
                copy.start()

    for cut in range(X_CUTS):
        x_copy(cut).start()

    @pl.when(flag[0] == 1)
    def _():
        start(own, crossed)

    @pl.when(flag[0] != 1)
    def _():
        start(near, far)

    for cut in range(X_CUTS):
        x_copy(cut).wait()
    acts = []
    for side in range(2):
        vals = []
        for part in range(2):
            for cut in range(CUTS):
                in_copy(side, own, part, cut).wait()
            vals.append(
                jnp.dot(x_buf[...], in_buf[2 * side + part], preferred_element_type=jnp.float32)
            )
        gate_val, up_val = vals
        acts.append((gate_val / (1.0 + jnp.exp(-gate_val)) * up_val).astype(jnp.bfloat16))
    act = jnp.concatenate(acts, axis=1)
    copies = []
    for step in range(OUT_STEPS):
        columns = slice(step * wide, (step + 1) * wide)
        for copy in down_copies(own, crossed, step):
            copy.wait()
        rows_out = jnp.dot(act, down_buf[:, columns], preferred_element_type=jnp.float32)
        for chunk in range(out.shape[0]):
            y_buf[chunk, :, columns] = rows_out[chunk * CAP : (chunk + 1) * CAP].astype(
                jnp.bfloat16
            )
        copy = pltpu.make_async_copy(
            y_buf.at[:, :, pl.ds(step * wide, wide)],
            out.at[:, :, pl.ds(step * wide, wide)],
            y_sem.at[step],
        )
        copy.start()
        copies.append(copy)
    for copy in copies:
        copy.wait()


def expert_ffn(flag, rows_in, own, crossed, near, far):
    count = rows_in.shape[0]
    hf = own[0].shape[2]
    return pl.pallas_call(
        ffn_kernel,
        out_shape=jax.ShapeDtypeStruct((count // CAP, CAP, D), jnp.bfloat16),
        in_specs=[pl.BlockSpec(memory_space=pltpu.SMEM)]
        + [pl.BlockSpec(memory_space=pltpu.HBM)] * 15,
        out_specs=pl.BlockSpec(memory_space=pltpu.HBM),
        scratch_shapes=[
            pltpu.VMEM((count, D), jnp.bfloat16),
            pltpu.VMEM((4, D, hf), jnp.bfloat16),
            pltpu.VMEM((2 * hf, D), jnp.bfloat16),
            pltpu.VMEM((count // CAP, CAP, D), jnp.bfloat16),
            pltpu.SemaphoreType.DMA((X_CUTS,)),
            pltpu.SemaphoreType.DMA((4, CUTS)),
            pltpu.SemaphoreType.DMA((4, OUT_STEPS)),
            pltpu.SemaphoreType.DMA((OUT_STEPS,)),
        ],
        compiler_params=pltpu.CompilerParams(vmem_limit_bytes=123 * 512 * 1024),
        cost_estimate=pl.CostEstimate(
            flops=12 * count * D * hf, bytes_accessed=12 * D * hf + 4 * count * D, transcendentals=0
        ),
        name="expert_ffn",
    )(flag, rows_in, *own, *crossed, *near, *far)


def combine_kernel(weights, rows_in, hidden, out):
    flat = jnp.concatenate([rows_in[chunk] for chunk in range(rows_in.shape[0])], axis=0)
    out[...] = hidden[...] + jnp.dot(weights[...], flat, preferred_element_type=jnp.float32)


def combined(weights, rows_in, hidden):
    chunks, each, _ = rows_in.shape
    rows = hidden.shape[0]
    wide = D // COMBINE_STEPS
    return pl.pallas_call(
        combine_kernel,
        grid=(COMBINE_STEPS,),
        out_shape=jax.ShapeDtypeStruct((rows, D), jnp.float32),
        in_specs=[
            pl.BlockSpec((rows, chunks * each), lambda i: (0, 0)),
            pl.BlockSpec((chunks, each, wide), lambda i: (0, 0, i)),
            pl.BlockSpec((rows, wide), lambda i: (0, i)),
        ],
        out_specs=pl.BlockSpec((rows, wide), lambda i: (0, i)),
        compiler_params=pltpu.CompilerParams(
            dimension_semantics=("arbitrary",), vmem_limit_bytes=123 * 512 * 1024
        ),
        cost_estimate=pl.CostEstimate(
            flops=2 * rows * chunks * each * D, bytes_accessed=2 * chunks * each * D, transcendentals=0
        ),
        name="combined",
    )(weights, rows_in, hidden)


def local(
    resid,
    queries,
    new_keys,
    new_values,
    cache_keys,
    cache_values,
    cache_len,
    out_proj,
    norm_gain,
    router,
    expert_ids,
    gate_slab,
    up_slab,
    down_slab,
):
    rows = resid.shape[0]
    chips = lax.axis_size("chip")
    core = lax.axis_index("core")
    depth = lax.axis_index("dp")
    depths = lax.axis_size("dp")

    other_proj = flipped(out_proj, "core", 1)
    spots = [(c, d) for c in range(2) for d in range(depths)]
    across = [(c * depths + d, c * depths + (d ^ 1)) for c, d in spots if c != d % 2]
    beside = [(c * depths + d, (1 - c) * depths + d) for c, d in spots if c == d % 2]

    def moved(slab, pairs, after=None):
        if after is not None:
            slab, _ = lax.optimization_barrier((slab, after))
        return lax.ppermute(slab, ("core", "dp"), pairs)

    gate_crossed = moved(gate_slab, across)
    gate_near = moved(gate_slab, beside)
    up_near = moved(up_slab, beside)
    down_near = moved(down_slab, beside)
    flag = (core == depth % 2).astype(jnp.int32).reshape(1)
    ring = [(c * depths + d, c * depths + (d + 1 - 2 * c) % depths) for c, d in spots]

    def gathered(value):
        blocks = [value]
        for _ in range(depths - 1):
            blocks.append(lax.ppermute(blocks[-1], ("core", "dp"), ring))
        return blocks

    id_blocks = gathered(expert_ids)
    ids = jnp.concatenate(id_blocks, axis=0)

    piece = out_proj.shape[0]
    sent = attention(
        core.astype(jnp.int32).reshape(1),
        queries,
        new_keys,
        new_values,
        cache_keys,
        cache_values,
        cache_len,
        chips,
    )
    regrouped = lax.all_to_all(sent, "chip", split_axis=0, concat_axis=0, tiled=True)
    regrouped = regrouped.reshape(chips * rows, 2 * piece)
    partial = jnp.dot(regrouped[:, :piece], out_proj, preferred_element_type=jnp.float32)
    partial = partial + jnp.dot(
        regrouped[:, piece:], other_proj, preferred_element_type=jnp.float32
    )
    count = ids.shape[0]
    labels = 4 * jnp.arange(chips, dtype=jnp.int32) + 2 * (depth % 2) + depth // 2
    hits = ids.T[:, None, :] == labels[None, :, None]
    member = jnp.any(hits, axis=0)
    at = jnp.arange(count, dtype=jnp.int32)
    before = (at[:, None] < at[None, :]) & (at[:, None] // rows == at[None, :] // rows)
    rank = jnp.dot(
        member.astype(jnp.bfloat16),
        before.astype(jnp.bfloat16),
        preferred_element_type=jnp.float32,
    ).astype(jnp.int32)
    source = (depth + depths + (2 * core - 1) * (at // rows)) % depths
    place = jnp.where(member, rank + CAP * source[None, :], -1)
    slots = CAP * depths
    dispatch = place[:, None, :] == jnp.arange(slots, dtype=jnp.int32)[None, :, None]

    chunk = jnp.arange(chips * depths, dtype=jnp.int32)
    homes = 4 * (chunk // depths) + 2 * (chunk % 2) + (chunk % depths) // 2
    own_hits = expert_ids[:, :, None] == homes[None, None, :]
    own_member = jnp.any(own_hits, axis=1)
    turn = jnp.arange(rows, dtype=jnp.int32)
    own_rank = jnp.dot(
        (turn[None, :] < turn[:, None]).astype(jnp.bfloat16),
        own_member.astype(jnp.bfloat16),
        preferred_element_type=jnp.float32,
    ).astype(jnp.int32)
    own_rank = jnp.where(own_member, own_rank, -1)
    own_slots = own_rank[:, :, None] == jnp.arange(CAP, dtype=jnp.int32)[None, None, :]

    partial = partial.astype(jnp.bfloat16)
    up_crossed = moved(up_slab, across, partial)
    middle = down_slab.shape[1] // 2
    held, _ = lax.optimization_barrier((down_slab, partial))
    halves = lax.optimization_barrier((held[:, :middle], held[:, middle:]))
    down_crossed = [moved(half, across) for half in halves]
    partial = lax.all_to_all(
        partial.reshape(chips, rows, D), "chip", split_axis=0, concat_axis=0, tiled=True
    )
    partial, dispatch, own_slots = lax.optimization_barrier((partial, dispatch, own_slots))
    hidden = resid.astype(jnp.float32) + jnp.sum(partial.astype(jnp.float32), axis=0)
    meansq = jnp.mean(hidden * hidden, axis=1, keepdims=True)
    normed = (hidden * lax.rsqrt(jnp.maximum(meansq, 0.25)) * norm_gain).astype(jnp.bfloat16)

    tokens = jnp.concatenate(gathered(normed), axis=0)
    outgoing = jnp.dot(
        dispatch.reshape(chips * slots, count).astype(jnp.bfloat16),
        tokens,
        preferred_element_type=jnp.float32,
    ).astype(jnp.bfloat16)
    gate_far = moved(gate_crossed, beside, outgoing)
    up_far = moved(up_crossed, beside, outgoing)
    down_far = [moved(half, beside, outgoing) for half in down_crossed]
    incoming = lax.all_to_all(
        outgoing.reshape(chips, slots, D), "chip", split_axis=0, concat_axis=0, tiled=True
    )

    logits = jnp.dot(normed, router, preferred_element_type=jnp.float32)
    experts = router.shape[1]
    onehot = expert_ids[:, :, None] == jnp.arange(experts, dtype=jnp.int32)[None, None, :]
    chosen = jnp.sum(jnp.where(onehot, logits[:, None, :], 0.0), axis=2)
    peak_logit = jnp.max(chosen, axis=1, keepdims=True)
    exp_logit = jnp.exp(chosen - peak_logit)
    gate_probs = (exp_logit / jnp.sum(exp_logit, axis=1, keepdims=True)).astype(jnp.bfloat16)
    spread = jnp.sum(jnp.where(own_hits, gate_probs.astype(jnp.float32)[:, :, None], 0.0), axis=1)
    combine = jnp.where(own_slots, spread[:, :, None], 0.0).astype(jnp.bfloat16)

    produced = expert_ffn(
        flag,
        incoming.reshape(chips * slots, D),
        (gate_slab, up_slab, down_slab),
        (gate_crossed, up_crossed, *down_crossed),
        (gate_near, up_near, down_near),
        (gate_far, up_far, *down_far),
    )
    returned = lax.all_to_all(produced, ("chip", "dp"), split_axis=0, concat_axis=0, tiled=True)
    return combined(combine.reshape(rows, chips * depths * CAP), returned, hidden)


def solution(mesh):
    split = Mesh(mesh.devices.reshape(-1, 2, mesh.shape["dp"]), ALL)
    in_specs = (
        P(ALL, None),
        P(ALL, None),
        P(ALL, None),
        P(ALL, None),
        P(ALL, None, None),
        P(ALL, None, None),
        P(ALL),
        P(EP, None),
        P(),
        P(),
        P(ALL, None),
        P(ALL, None, None),
        P(ALL, None, None),
        P(ALL, None, None),
    )

    return jax.shard_map(
        local, mesh=split, in_specs=in_specs, out_specs=P(ALL, None), check_vma=False
    )
```

```python
import math

import jax
import jax.numpy as jnp
from jax import lax
from jax.experimental import pallas as pl
from jax.experimental.pallas import tpu as pltpu
from jax.sharding import Mesh
from jax.sharding import PartitionSpec as P

D = 4096
H = 64
KVH = 4
HD = 128
CAP = 4
ATTN_STEPS = 2
OUT_STEPS = 2
CUTS = 8
X_CUTS = 4
COMBINE_STEPS = 2


EP = ("chip", "core")
ALL = ("chip", "core", "dp")


def flipped(value, axis, mask):
    pairs = [(source, source ^ mask) for source in range(lax.axis_size(axis))]
    return lax.ppermute(value, axis, pairs)


def attention_kernel(swap, lengths, q_in, nk_in, nv_in, keys, values, out, q_buf, o_buf):
    step = pl.program_id(0)
    tokens = q_in.shape[0]
    group = H // KVH
    scale = 1.0 / math.sqrt(HD)

    @pl.when(step == 0)
    def _():
        for head in range(H):
            q_buf[pl.ds(head, tokens, stride=H), :] = q_in[:, head * HD : (head + 1) * HD].astype(
                jnp.float32
            )

    nk = nk_in[...].astype(jnp.float32)
    nv = nv_in[...].astype(jnp.float32)
    span = keys.shape[1]
    owner = lax.broadcasted_iota(jnp.int32, (H, HD), 0) // group
    position = lax.broadcasted_iota(jnp.int32, (H, span), 1)
    each = keys.shape[0]
    base = step * each
    q_all = q_buf[pl.ds(base * H, each * H), :]

    def fanned(value):
        return jnp.concatenate(
            [
                jnp.broadcast_to(value[row : row + 1, g * HD : (g + 1) * HD], (group, HD))
                for row in range(each)
                for g in range(KVH)
            ],
            axis=0,
        )

    past = []
    for row in range(each):
        q = q_all[row * H : (row + 1) * H]
        blocks = [jnp.where(owner == g, q, 0.0).astype(jnp.bfloat16) for g in range(KVH)]
        scores = scale * lax.dot_general(
            jnp.concatenate(blocks, axis=1),
            keys[row],
            (((1,), (1,)), ((), ())),
            preferred_element_type=jnp.float32,
        )
        past.append(jnp.where(position < lengths[base + row], scores, -1e30))
    past = jnp.concatenate(past, axis=0)
    own = scale * jnp.sum(q_all * fanned(nk), axis=1, keepdims=True)
    peak = jnp.maximum(jnp.max(past, axis=1, keepdims=True), own)
    past_exp = jnp.exp(past - peak)
    own_exp = jnp.exp(own - peak)
    denom = jnp.sum(past_exp, axis=1, keepdims=True) + own_exp
    weights = (past_exp / denom).astype(jnp.bfloat16)
    own_part = (own_exp / denom).astype(jnp.bfloat16).astype(jnp.float32) * fanned(nv)
    for row in range(each):
        wide = jnp.dot(
            weights[row * H : (row + 1) * H], values[row], preferred_element_type=jnp.float32
        )
        blended = jnp.concatenate(
            [wide[g * group : (g + 1) * group, g * HD : (g + 1) * HD] for g in range(KVH)], axis=0
        )
        o_buf[pl.ds((base + row) * H, H), :] = blended + own_part[row * H : (row + 1) * H]

    @pl.when(step == pl.num_programs(0) - 1)
    def _():
        chips, _, width = out.shape
        per = width // HD
        for chip in range(chips):
            for at in range(per):
                head = chip * per + at
                first = o_buf[pl.ds(head, tokens, stride=H), :]
                second = o_buf[pl.ds(chip * per + (at ^ (per // 2)), tokens, stride=H), :]
                out[chip, :, at * HD : (at + 1) * HD] = jnp.where(
                    swap[0] == 1, second, first
                ).astype(jnp.bfloat16)


def attention(swap, queries, new_keys, new_values, cache_keys, cache_values, cache_len, chips):
    rows = queries.shape[0]
    span = cache_keys.shape[1]
    each = rows // ATTN_STEPS
    smem = pl.BlockSpec(memory_space=pltpu.SMEM)
    return pl.pallas_call(
        attention_kernel,
        grid=(ATTN_STEPS,),
        out_shape=jax.ShapeDtypeStruct((chips, rows, H * HD // chips), jnp.bfloat16),
        in_specs=[
            smem,
            smem,
            pl.BlockSpec((rows, H * HD), lambda i: (0, 0)),
            pl.BlockSpec((each, KVH * HD), lambda i: (i, 0)),
            pl.BlockSpec((each, KVH * HD), lambda i: (i, 0)),
            pl.BlockSpec((each, span, KVH * HD), lambda i: (i, 0, 0)),
            pl.BlockSpec((each, span, KVH * HD), lambda i: (i, 0, 0)),
        ],
        out_specs=pl.BlockSpec((chips, rows, H * HD // chips), lambda i: (0, 0, 0)),
        scratch_shapes=[
            pltpu.VMEM((rows * H, HD), jnp.float32),
            pltpu.VMEM((rows * H, HD), jnp.float32),
        ],
        compiler_params=pltpu.CompilerParams(dimension_semantics=("arbitrary",)),
        cost_estimate=pl.CostEstimate(
            flops=8 * rows * H * HD * span, bytes_accessed=4 * rows * span * KVH * HD, transcendentals=0
        ),
        name="attention",
    )(swap, cache_len, queries, new_keys, new_values, cache_keys, cache_values)


def ffn_kernel(flag, rows_in, *refs):
    own, crossed, near, far = refs[0:3], refs[3:7], refs[7:10], refs[10:14]
    out, x_buf, in_buf, down_buf, y_buf, x_sem, in_sem, down_sem, y_sem = refs[14:]
    hf = own[0].shape[2]
    deep = D // CUTS
    wide = D // OUT_STEPS

    def x_copy(cut):
        part = pl.ds(cut * rows_in.shape[0] // X_CUTS, rows_in.shape[0] // X_CUTS)
        return pltpu.make_async_copy(rows_in.at[part], x_buf.at[part], x_sem.at[cut])

    def in_copy(side, source, part, cut):
        return pltpu.make_async_copy(
            source[part].at[0, pl.ds(cut * deep, deep)],
            in_buf.at[2 * side + part, pl.ds(cut * deep, deep)],
            in_sem.at[2 * side + part, cut],
        )

    def down_copy(row, source, step):
        return pltpu.make_async_copy(
            source.at[0, :, pl.ds(step * wide, wide)],
            down_buf.at[pl.ds(row, source.shape[1]), pl.ds(step * wide, wide)],
            down_sem.at[(4 * row) // hf, step],
        )

    def down_copies(first, second, step):
        return (
            down_copy(0, first[2], step),
            down_copy(hf, second[2], step),
            down_copy(hf + second[2].shape[1], second[3], step),
        )

    def start(first, second):
        for side, source in ((0, first), (1, second)):
            for part in range(2):
                for cut in range(CUTS):
                    in_copy(side, source, part, cut).start()
        for step in range(OUT_STEPS):
            for copy in down_copies(first, second, step):
                copy.start()

    for cut in range(X_CUTS):
        x_copy(cut).start()

    @pl.when(flag[0] == 1)
    def _():
        start(own, crossed)

    @pl.when(flag[0] != 1)
    def _():
        start(near, far)

    for cut in range(X_CUTS):
        x_copy(cut).wait()
    acts = []
    for side in range(2):
        vals = []
        for part in range(2):
            for cut in range(CUTS):
                in_copy(side, own, part, cut).wait()
            vals.append(
                jnp.dot(x_buf[...], in_buf[2 * side + part], preferred_element_type=jnp.float32)
            )
        gate_val, up_val = vals
        acts.append((gate_val / (1.0 + jnp.exp(-gate_val)) * up_val).astype(jnp.bfloat16))
    act = jnp.concatenate(acts, axis=1)
    copies = []
    for step in range(OUT_STEPS):
        columns = slice(step * wide, (step + 1) * wide)
        for copy in down_copies(own, crossed, step):
            copy.wait()
        rows_out = jnp.dot(act, down_buf[:, columns], preferred_element_type=jnp.float32)
        for chunk in range(out.shape[0]):
            y_buf[chunk, :, columns] = rows_out[chunk * CAP : (chunk + 1) * CAP].astype(
                jnp.bfloat16
            )
        copy = pltpu.make_async_copy(
            y_buf.at[:, :, pl.ds(step * wide, wide)],
            out.at[:, :, pl.ds(step * wide, wide)],
            y_sem.at[step],
        )
        copy.start()
        copies.append(copy)
    for copy in copies:
        copy.wait()


def expert_ffn(flag, rows_in, own, crossed, near, far):
    count = rows_in.shape[0]
    hf = own[0].shape[2]
    return pl.pallas_call(
        ffn_kernel,
        out_shape=jax.ShapeDtypeStruct((count // CAP, CAP, D), jnp.bfloat16),
        in_specs=[pl.BlockSpec(memory_space=pltpu.SMEM)]
        + [pl.BlockSpec(memory_space=pltpu.HBM)] * 15,
        out_specs=pl.BlockSpec(memory_space=pltpu.HBM),
        scratch_shapes=[
            pltpu.VMEM((count, D), jnp.bfloat16),
            pltpu.VMEM((4, D, hf), jnp.bfloat16),
            pltpu.VMEM((2 * hf, D), jnp.bfloat16),
            pltpu.VMEM((count // CAP, CAP, D), jnp.bfloat16),
            pltpu.SemaphoreType.DMA((X_CUTS,)),
            pltpu.SemaphoreType.DMA((4, CUTS)),
            pltpu.SemaphoreType.DMA((8, OUT_STEPS)),
            pltpu.SemaphoreType.DMA((OUT_STEPS,)),
        ],
        compiler_params=pltpu.CompilerParams(vmem_limit_bytes=123 * 512 * 1024),
        cost_estimate=pl.CostEstimate(
            flops=12 * count * D * hf, bytes_accessed=12 * D * hf + 4 * count * D, transcendentals=0
        ),
        name="expert_ffn",
    )(flag, rows_in, *own, *crossed, *near, *far)


def combine_kernel(weights, rows_in, hidden, out):
    flat = jnp.concatenate([rows_in[chunk] for chunk in range(rows_in.shape[0])], axis=0)
    out[...] = hidden[...] + jnp.dot(weights[...], flat, preferred_element_type=jnp.float32)


def combined(weights, rows_in, hidden):
    chunks, each, _ = rows_in.shape
    rows = hidden.shape[0]
    wide = D // COMBINE_STEPS
    return pl.pallas_call(
        combine_kernel,
        grid=(COMBINE_STEPS,),
        out_shape=jax.ShapeDtypeStruct((rows, D), jnp.float32),
        in_specs=[
            pl.BlockSpec((rows, chunks * each), lambda i: (0, 0)),
            pl.BlockSpec((chunks, each, wide), lambda i: (0, 0, i)),
            pl.BlockSpec((rows, wide), lambda i: (0, i)),
        ],
        out_specs=pl.BlockSpec((rows, wide), lambda i: (0, i)),
        compiler_params=pltpu.CompilerParams(
            dimension_semantics=("arbitrary",), vmem_limit_bytes=123 * 512 * 1024
        ),
        cost_estimate=pl.CostEstimate(
            flops=2 * rows * chunks * each * D, bytes_accessed=2 * chunks * each * D, transcendentals=0
        ),
        name="combined",
    )(weights, rows_in, hidden)


def local(
    resid,
    queries,
    new_keys,
    new_values,
    cache_keys,
    cache_values,
    cache_len,
    out_proj,
    norm_gain,
    router,
    expert_ids,
    gate_slab,
    up_slab,
    down_slab,
):
    rows = resid.shape[0]
    chips = lax.axis_size("chip")
    core = lax.axis_index("core")
    depth = lax.axis_index("dp")
    depths = lax.axis_size("dp")

    other_proj = flipped(out_proj, "core", 1)
    spots = [(c, d) for c in range(2) for d in range(depths)]
    across = [(c * depths + d, c * depths + (d ^ 1)) for c, d in spots if c != d % 2]
    beside = [(c * depths + d, (1 - c) * depths + d) for c, d in spots if c == d % 2]

    def moved(slab, pairs, after=None):
        if after is not None:
            slab, _ = lax.optimization_barrier((slab, after))
        return lax.ppermute(slab, ("core", "dp"), pairs)

    gate_crossed = moved(gate_slab, across)
    gate_near = moved(gate_slab, beside)
    up_near = moved(up_slab, beside)
    down_near = moved(down_slab, beside)
    flag = (core == depth % 2).astype(jnp.int32).reshape(1)
    ring = [(c * depths + d, c * depths + (d + 1 - 2 * c) % depths) for c, d in spots]

    def gathered(value):
        blocks = [value]
        for _ in range(depths - 1):
            blocks.append(lax.ppermute(blocks[-1], ("core", "dp"), ring))
        return blocks

    id_blocks = gathered(expert_ids)
    ids = jnp.concatenate(id_blocks, axis=0)

    piece = out_proj.shape[0]
    sent = attention(
        core.astype(jnp.int32).reshape(1),
        queries,
        new_keys,
        new_values,
        cache_keys,
        cache_values,
        cache_len,
        chips,
    )
    regrouped = lax.all_to_all(sent, "chip", split_axis=0, concat_axis=0, tiled=True)
    regrouped = regrouped.reshape(chips * rows, 2 * piece)
    partial = jnp.dot(regrouped[:, :piece], out_proj, preferred_element_type=jnp.float32)
    partial = partial + jnp.dot(
        regrouped[:, piece:], other_proj, preferred_element_type=jnp.float32
    )
    count = ids.shape[0]
    labels = 4 * jnp.arange(chips, dtype=jnp.int32) + 2 * (depth % 2) + depth // 2
    hits = ids.T[:, None, :] == labels[None, :, None]
    member = jnp.any(hits, axis=0)
    at = jnp.arange(count, dtype=jnp.int32)
    before = (at[:, None] < at[None, :]) & (at[:, None] // rows == at[None, :] // rows)
    rank = jnp.dot(
        member.astype(jnp.bfloat16),
        before.astype(jnp.bfloat16),
        preferred_element_type=jnp.float32,
    ).astype(jnp.int32)
    source = (depth + depths + (2 * core - 1) * (at // rows)) % depths
    place = jnp.where(member, rank + CAP * source[None, :], -1)
    slots = CAP * depths
    dispatch = place[:, None, :] == jnp.arange(slots, dtype=jnp.int32)[None, :, None]

    chunk = jnp.arange(chips * depths, dtype=jnp.int32)
    homes = 4 * (chunk // depths) + 2 * (chunk % 2) + (chunk % depths) // 2
    own_hits = expert_ids[:, :, None] == homes[None, None, :]
    own_member = jnp.any(own_hits, axis=1)
    turn = jnp.arange(rows, dtype=jnp.int32)
    own_rank = jnp.dot(
        (turn[None, :] < turn[:, None]).astype(jnp.bfloat16),
        own_member.astype(jnp.bfloat16),
        preferred_element_type=jnp.float32,
    ).astype(jnp.int32)
    own_rank = jnp.where(own_member, own_rank, -1)
    own_slots = own_rank[:, :, None] == jnp.arange(CAP, dtype=jnp.int32)[None, None, :]

    partial = partial.astype(jnp.bfloat16)
    up_crossed = moved(up_slab, across, partial)
    middle = down_slab.shape[1] // 4 * 3
    held, _ = lax.optimization_barrier((down_slab, partial))
    halves = lax.optimization_barrier((held[:, :middle], held[:, middle:]))
    most = moved(halves[0], across)
    rest = moved(halves[1], across)
    down_crossed = (most, rest)
    partial = lax.all_to_all(
        partial.reshape(chips, rows, D), "chip", split_axis=0, concat_axis=0, tiled=True
    )
    partial, dispatch, own_slots = lax.optimization_barrier((partial, dispatch, own_slots))
    hidden = resid.astype(jnp.float32) + jnp.sum(partial.astype(jnp.float32), axis=0)
    meansq = jnp.mean(hidden * hidden, axis=1, keepdims=True)
    normed = (hidden * lax.rsqrt(jnp.maximum(meansq, 0.25)) * norm_gain).astype(jnp.bfloat16)

    blocks = gathered(normed)
    tokens = jnp.concatenate(blocks, axis=0)
    outgoing = jnp.dot(
        dispatch.reshape(chips * slots, count).astype(jnp.bfloat16),
        tokens,
        preferred_element_type=jnp.float32,
    ).astype(jnp.bfloat16)
    gate_far = moved(gate_crossed, beside, outgoing)
    up_far = moved(up_crossed, beside, outgoing)
    down_far = [moved(half, beside, outgoing) for half in down_crossed]
    incoming = lax.all_to_all(
        outgoing.reshape(chips, slots, D), "chip", split_axis=0, concat_axis=0, tiled=True
    )

    logits = jnp.dot(normed, router, preferred_element_type=jnp.float32)
    experts = router.shape[1]
    onehot = expert_ids[:, :, None] == jnp.arange(experts, dtype=jnp.int32)[None, None, :]
    chosen = jnp.sum(jnp.where(onehot, logits[:, None, :], 0.0), axis=2)
    peak_logit = jnp.max(chosen, axis=1, keepdims=True)
    exp_logit = jnp.exp(chosen - peak_logit)
    gate_probs = (exp_logit / jnp.sum(exp_logit, axis=1, keepdims=True)).astype(jnp.bfloat16)
    spread = jnp.sum(jnp.where(own_hits, gate_probs.astype(jnp.float32)[:, :, None], 0.0), axis=1)
    combine = jnp.where(own_slots, spread[:, :, None], 0.0).astype(jnp.bfloat16)

    produced = expert_ffn(
        flag,
        incoming.reshape(chips * slots, D),
        (gate_slab, up_slab, down_slab),
        (gate_crossed, up_crossed, *down_crossed),
        (gate_near, up_near, down_near),
        (gate_far, up_far, *down_far),
    )
    returned = lax.all_to_all(produced, ("chip", "dp"), split_axis=0, concat_axis=0, tiled=True)
    return combined(combine.reshape(rows, chips * depths * CAP), returned, hidden)


def solution(mesh):
    split = Mesh(mesh.devices.reshape(-1, 2, mesh.shape["dp"]), ALL)
    in_specs = (
        P(ALL, None),
        P(ALL, None),
        P(ALL, None),
        P(ALL, None),
        P(ALL, None, None),
        P(ALL, None, None),
        P(ALL),
        P(EP, None),
        P(),
        P(),
        P(ALL, None),
        P(ALL, None, None),
        P(ALL, None, None),
        P(ALL, None, None),
    )

    return jax.shard_map(
        local, mesh=split, in_specs=in_specs, out_specs=P(ALL, None), check_vma=False
    )
```

```python
import math

import jax
import jax.numpy as jnp
from jax import lax
from jax.experimental import pallas as pl
from jax.experimental.pallas import tpu as pltpu
from jax.sharding import Mesh
from jax.sharding import PartitionSpec as P

D = 4096
H = 64
KVH = 4
HD = 128
CAP = 4
ATTN_STEPS = 2
OUT_STEPS = 4
CUTS = 1
X_CUTS = 1
AHEAD = 2
COMBINE_STEPS = 2


EP = ("chip", "core")
ALL = ("chip", "core", "dp")


def flipped(value, axis, mask):
    pairs = [(source, source ^ mask) for source in range(lax.axis_size(axis))]
    return lax.ppermute(value, axis, pairs)


def attention_kernel(swap, lengths, q_in, nk_in, nv_in, keys, values, out, q_buf, o_buf):
    step = pl.program_id(0)
    tokens = q_in.shape[0]
    group = H // KVH
    scale = 1.0 / math.sqrt(HD)

    @pl.when(step == 0)
    def _():
        for head in range(H):
            q_buf[pl.ds(head, tokens, stride=H), :] = q_in[:, head * HD : (head + 1) * HD].astype(
                jnp.float32
            )

    nk = nk_in[...].astype(jnp.float32)
    nv = nv_in[...].astype(jnp.float32)
    span = keys.shape[1]
    owner = lax.broadcasted_iota(jnp.int32, (H, HD), 0) // group
    position = lax.broadcasted_iota(jnp.int32, (H, span), 1)
    each = keys.shape[0]
    base = step * each
    q_all = q_buf[pl.ds(base * H, each * H), :]

    def fanned(value):
        return jnp.concatenate(
            [
                jnp.broadcast_to(value[row : row + 1, g * HD : (g + 1) * HD], (group, HD))
                for row in range(each)
                for g in range(KVH)
            ],
            axis=0,
        )

    past = []
    for row in range(each):
        q = q_all[row * H : (row + 1) * H]
        blocks = [jnp.where(owner == g, q, 0.0).astype(jnp.bfloat16) for g in range(KVH)]
        scores = scale * lax.dot_general(
            jnp.concatenate(blocks, axis=1),
            keys[row],
            (((1,), (1,)), ((), ())),
            preferred_element_type=jnp.float32,
        )
        past.append(jnp.where(position < lengths[base + row], scores, -1e30))
    past = jnp.concatenate(past, axis=0)
    own = scale * jnp.sum(q_all * fanned(nk), axis=1, keepdims=True)
    peak = jnp.maximum(jnp.max(past, axis=1, keepdims=True), own)
    past_exp = jnp.exp(past - peak)
    own_exp = jnp.exp(own - peak)
    denom = jnp.sum(past_exp, axis=1, keepdims=True) + own_exp
    weights = (past_exp / denom).astype(jnp.bfloat16)
    own_part = (own_exp / denom).astype(jnp.bfloat16).astype(jnp.float32) * fanned(nv)
    for row in range(each):
        wide = jnp.dot(
            weights[row * H : (row + 1) * H], values[row], preferred_element_type=jnp.float32
        )
        blended = jnp.concatenate(
            [wide[g * group : (g + 1) * group, g * HD : (g + 1) * HD] for g in range(KVH)], axis=0
        )
        o_buf[pl.ds((base + row) * H, H), :] = blended + own_part[row * H : (row + 1) * H]

    @pl.when(step == pl.num_programs(0) - 1)
    def _():
        chips, _, width = out.shape
        per = width // HD
        for chip in range(chips):
            for at in range(per):
                head = chip * per + at
                first = o_buf[pl.ds(head, tokens, stride=H), :]
                second = o_buf[pl.ds(chip * per + (at ^ (per // 2)), tokens, stride=H), :]
                out[chip, :, at * HD : (at + 1) * HD] = jnp.where(
                    swap[0] == 1, second, first
                ).astype(jnp.bfloat16)


def attention(swap, queries, new_keys, new_values, cache_keys, cache_values, cache_len, chips):
    rows = queries.shape[0]
    span = cache_keys.shape[1]
    each = rows // ATTN_STEPS
    smem = pl.BlockSpec(memory_space=pltpu.SMEM)
    return pl.pallas_call(
        attention_kernel,
        grid=(ATTN_STEPS,),
        out_shape=jax.ShapeDtypeStruct((chips, rows, H * HD // chips), jnp.bfloat16),
        in_specs=[
            smem,
            smem,
            pl.BlockSpec((rows, H * HD), lambda i: (0, 0)),
            pl.BlockSpec((each, KVH * HD), lambda i: (i, 0)),
            pl.BlockSpec((each, KVH * HD), lambda i: (i, 0)),
            pl.BlockSpec((each, span, KVH * HD), lambda i: (i, 0, 0)),
            pl.BlockSpec((each, span, KVH * HD), lambda i: (i, 0, 0)),
        ],
        out_specs=pl.BlockSpec((chips, rows, H * HD // chips), lambda i: (0, 0, 0)),
        scratch_shapes=[
            pltpu.VMEM((rows * H, HD), jnp.float32),
            pltpu.VMEM((rows * H, HD), jnp.float32),
        ],
        compiler_params=pltpu.CompilerParams(dimension_semantics=("arbitrary",)),
        cost_estimate=pl.CostEstimate(
            flops=8 * rows * H * HD * span, bytes_accessed=4 * rows * span * KVH * HD, transcendentals=0
        ),
        name="attention",
    )(swap, cache_len, queries, new_keys, new_values, cache_keys, cache_values)


def ffn_kernel(flag, rows_in, *refs):
    own, crossed, near, far = refs[0:3], refs[3:7], refs[7:10], refs[10:14]
    out, x_buf, in_buf, down_buf, y_buf, x_sem, in_sem, down_sem, y_sem = refs[14:]
    hf = own[0].shape[2]
    deep = D // CUTS
    wide = D // OUT_STEPS

    def x_copy(cut):
        part = pl.ds(cut * rows_in.shape[0] // X_CUTS, rows_in.shape[0] // X_CUTS)
        return pltpu.make_async_copy(rows_in.at[part], x_buf.at[part], x_sem.at[cut])

    def in_copy(side, source, part, cut):
        return pltpu.make_async_copy(
            source[part].at[0, pl.ds(cut * deep, deep)],
            in_buf.at[2 * side + part, pl.ds(cut * deep, deep)],
            in_sem.at[2 * side + part, cut],
        )

    def down_copy(row, source, step):
        return pltpu.make_async_copy(
            source.at[0, :, pl.ds(step * wide, wide)],
            down_buf.at[pl.ds(row, source.shape[1]), pl.ds(step * wide, wide)],
            down_sem.at[(4 * row) // hf, step],
        )

    def down_copies(first, second, step):
        return (
            down_copy(0, first[2], step),
            down_copy(hf, second[2], step),
            down_copy(hf + second[2].shape[1], second[3], step),
        )

    def slab(first, second, at):
        for cut in range(CUTS):
            in_copy(at // 2, (first, second)[at // 2], at % 2, cut).start()

    def downs(first, second, at):
        for step in range(OUT_STEPS):
            for copy in down_copies(first, second, step):
                copy.start()

    def start(task, at):
        @pl.when(flag[0] == 1)
        def _():
            task(own, crossed, at)

        @pl.when(flag[0] != 1)
        def _():
            task(near, far, at)

    for cut in range(X_CUTS):
        x_copy(cut).start()
    for at in range(AHEAD):
        start(slab, at)
    for cut in range(X_CUTS):
        x_copy(cut).wait()
    acts = []
    for side in range(2):
        vals = []
        for part in range(2):
            at = 2 * side + part
            for cut in range(CUTS):
                in_copy(side, own, part, cut).wait()
            if at + AHEAD < 4:
                start(slab, at + AHEAD)
            elif at + AHEAD == 4:
                start(downs, 0)
            vals.append(jnp.dot(x_buf[...], in_buf[at], preferred_element_type=jnp.float32))
        gate_val, up_val = vals
        acts.append((gate_val / (1.0 + jnp.exp(-gate_val)) * up_val).astype(jnp.bfloat16))
    act = jnp.concatenate(acts, axis=1)
    copies = []
    for step in range(OUT_STEPS):
        columns = slice(step * wide, (step + 1) * wide)
        for copy in down_copies(own, crossed, step):
            copy.wait()
        rows_out = jnp.dot(act, down_buf[:, columns], preferred_element_type=jnp.float32)
        for chunk in range(out.shape[0]):
            y_buf[chunk, :, columns] = rows_out[chunk * CAP : (chunk + 1) * CAP].astype(
                jnp.bfloat16
            )
        copy = pltpu.make_async_copy(
            y_buf.at[:, :, pl.ds(step * wide, wide)],
            out.at[:, :, pl.ds(step * wide, wide)],
            y_sem.at[step],
        )
        copy.start()
        copies.append(copy)
    for copy in copies:
        copy.wait()


def expert_ffn(flag, rows_in, own, crossed, near, far):
    count = rows_in.shape[0]
    hf = own[0].shape[2]
    return pl.pallas_call(
        ffn_kernel,
        out_shape=jax.ShapeDtypeStruct((count // CAP, CAP, D), jnp.bfloat16),
        in_specs=[pl.BlockSpec(memory_space=pltpu.SMEM)]
        + [pl.BlockSpec(memory_space=pltpu.HBM)] * 15,
        out_specs=pl.BlockSpec(memory_space=pltpu.HBM),
        scratch_shapes=[
            pltpu.VMEM((count, D), jnp.bfloat16),
            pltpu.VMEM((4, D, hf), jnp.bfloat16),
            pltpu.VMEM((2 * hf, D), jnp.bfloat16),
            pltpu.VMEM((count // CAP, CAP, D), jnp.bfloat16),
            pltpu.SemaphoreType.DMA((X_CUTS,)),
            pltpu.SemaphoreType.DMA((4, CUTS)),
            pltpu.SemaphoreType.DMA((8, OUT_STEPS)),
            pltpu.SemaphoreType.DMA((OUT_STEPS,)),
        ],
        compiler_params=pltpu.CompilerParams(vmem_limit_bytes=123 * 512 * 1024),
        cost_estimate=pl.CostEstimate(
            flops=12 * count * D * hf, bytes_accessed=12 * D * hf + 4 * count * D, transcendentals=0
        ),
        name="expert_ffn",
    )(flag, rows_in, *own, *crossed, *near, *far)


def combine_kernel(weights, rows_in, hidden, out):
    flat = jnp.concatenate([rows_in[chunk] for chunk in range(rows_in.shape[0])], axis=0)
    out[...] = hidden[...] + jnp.dot(weights[...], flat, preferred_element_type=jnp.float32)


def combined(weights, rows_in, hidden):
    chunks, each, _ = rows_in.shape
    rows = hidden.shape[0]
    wide = D // COMBINE_STEPS
    return pl.pallas_call(
        combine_kernel,
        grid=(COMBINE_STEPS,),
        out_shape=jax.ShapeDtypeStruct((rows, D), jnp.float32),
        in_specs=[
            pl.BlockSpec((rows, chunks * each), lambda i: (0, 0)),
            pl.BlockSpec((chunks, each, wide), lambda i: (0, 0, i)),
            pl.BlockSpec((rows, wide), lambda i: (0, i)),
        ],
        out_specs=pl.BlockSpec((rows, wide), lambda i: (0, i)),
        compiler_params=pltpu.CompilerParams(
            dimension_semantics=("arbitrary",), vmem_limit_bytes=123 * 512 * 1024
        ),
        cost_estimate=pl.CostEstimate(
            flops=2 * rows * chunks * each * D, bytes_accessed=2 * chunks * each * D, transcendentals=0
        ),
        name="combined",
    )(weights, rows_in, hidden)


def local(
    resid,
    queries,
    new_keys,
    new_values,
    cache_keys,
    cache_values,
    cache_len,
    out_proj,
    norm_gain,
    router,
    expert_ids,
    gate_slab,
    up_slab,
    down_slab,
):
    rows = resid.shape[0]
    chips = lax.axis_size("chip")
    core = lax.axis_index("core")
    depth = lax.axis_index("dp")
    depths = lax.axis_size("dp")

    other_proj = flipped(out_proj, "core", 1)
    spots = [(c, d) for c in range(2) for d in range(depths)]
    across = [(c * depths + d, c * depths + (d ^ 1)) for c, d in spots if c != d % 2]
    beside = [(c * depths + d, (1 - c) * depths + d) for c, d in spots if c == d % 2]

    def moved(slab, pairs, after=None):
        if after is not None:
            slab, _ = lax.optimization_barrier((slab, after))
        return lax.ppermute(slab, ("core", "dp"), pairs)

    gate_crossed = moved(gate_slab, across)
    gate_near = moved(gate_slab, beside)
    up_near = moved(up_slab, beside)
    down_near = moved(down_slab, beside)
    flag = (core == depth % 2).astype(jnp.int32).reshape(1)
    ring = [(c * depths + d, c * depths + (d + 1 - 2 * c) % depths) for c, d in spots]

    def gathered(value):
        blocks = [value]
        for _ in range(depths - 1):
            blocks.append(lax.ppermute(blocks[-1], ("core", "dp"), ring))
        return blocks

    id_blocks = gathered(expert_ids)
    ids = jnp.concatenate(id_blocks, axis=0)

    piece = out_proj.shape[0]
    sent = attention(
        core.astype(jnp.int32).reshape(1),
        queries,
        new_keys,
        new_values,
        cache_keys,
        cache_values,
        cache_len,
        chips,
    )
    regrouped = lax.all_to_all(sent, "chip", split_axis=0, concat_axis=0, tiled=True)
    regrouped = regrouped.reshape(chips * rows, 2 * piece)
    partial = jnp.dot(regrouped[:, :piece], out_proj, preferred_element_type=jnp.float32)
    partial = partial + jnp.dot(
        regrouped[:, piece:], other_proj, preferred_element_type=jnp.float32
    )
    count = ids.shape[0]
    labels = 4 * jnp.arange(chips, dtype=jnp.int32) + 2 * (depth % 2) + depth // 2
    hits = ids.T[:, None, :] == labels[None, :, None]
    member = jnp.any(hits, axis=0)
    at = jnp.arange(count, dtype=jnp.int32)
    before = (at[:, None] < at[None, :]) & (at[:, None] // rows == at[None, :] // rows)
    rank = jnp.dot(
        member.astype(jnp.bfloat16),
        before.astype(jnp.bfloat16),
        preferred_element_type=jnp.float32,
    ).astype(jnp.int32)
    source = (depth + depths + (2 * core - 1) * (at // rows)) % depths
    place = jnp.where(member, rank + CAP * source[None, :], -1)
    slots = CAP * depths
    dispatch = place[:, None, :] == jnp.arange(slots, dtype=jnp.int32)[None, :, None]

    chunk = jnp.arange(chips * depths, dtype=jnp.int32)
    homes = 4 * (chunk // depths) + 2 * (chunk % 2) + (chunk % depths) // 2
    own_hits = expert_ids[:, :, None] == homes[None, None, :]
    own_member = jnp.any(own_hits, axis=1)
    turn = jnp.arange(rows, dtype=jnp.int32)
    own_rank = jnp.dot(
        (turn[None, :] < turn[:, None]).astype(jnp.bfloat16),
        own_member.astype(jnp.bfloat16),
        preferred_element_type=jnp.float32,
    ).astype(jnp.int32)
    own_rank = jnp.where(own_member, own_rank, -1)
    own_slots = own_rank[:, :, None] == jnp.arange(CAP, dtype=jnp.int32)[None, None, :]

    partial = partial.astype(jnp.bfloat16)
    up_crossed = moved(up_slab, across, partial)
    middle = down_slab.shape[1] // 4 * 3
    held, _ = lax.optimization_barrier((down_slab, partial))
    halves = lax.optimization_barrier((held[:, :middle], held[:, middle:]))
    most = moved(halves[0], across)
    rest = moved(halves[1], across)
    down_crossed = (most, rest)
    partial = lax.all_to_all(
        partial.reshape(chips, rows, D), "chip", split_axis=0, concat_axis=0, tiled=True
    )
    partial, dispatch, own_slots = lax.optimization_barrier((partial, dispatch, own_slots))
    hidden = resid.astype(jnp.float32) + jnp.sum(partial.astype(jnp.float32), axis=0)
    meansq = jnp.mean(hidden * hidden, axis=1, keepdims=True)
    normed = (hidden * lax.rsqrt(jnp.maximum(meansq, 0.25)) * norm_gain).astype(jnp.bfloat16)

    blocks = gathered(normed)
    tokens = jnp.concatenate(blocks, axis=0)
    outgoing = jnp.dot(
        dispatch.reshape(chips * slots, count).astype(jnp.bfloat16),
        tokens,
        preferred_element_type=jnp.float32,
    ).astype(jnp.bfloat16)
    gate_far = moved(gate_crossed, beside, outgoing)
    up_far = moved(up_crossed, beside, outgoing)
    down_far = [moved(half, beside, outgoing) for half in down_crossed]
    incoming = lax.all_to_all(
        outgoing.reshape(chips, slots, D), "chip", split_axis=0, concat_axis=0, tiled=True
    )

    logits = jnp.dot(normed, router, preferred_element_type=jnp.float32)
    experts = router.shape[1]
    onehot = expert_ids[:, :, None] == jnp.arange(experts, dtype=jnp.int32)[None, None, :]
    chosen = jnp.sum(jnp.where(onehot, logits[:, None, :], 0.0), axis=2)
    peak_logit = jnp.max(chosen, axis=1, keepdims=True)
    exp_logit = jnp.exp(chosen - peak_logit)
    gate_probs = (exp_logit / jnp.sum(exp_logit, axis=1, keepdims=True)).astype(jnp.bfloat16)
    spread = jnp.sum(jnp.where(own_hits, gate_probs.astype(jnp.float32)[:, :, None], 0.0), axis=1)
    combine = jnp.where(own_slots, spread[:, :, None], 0.0).astype(jnp.bfloat16)

    produced = expert_ffn(
        flag,
        incoming.reshape(chips * slots, D),
        (gate_slab, up_slab, down_slab),
        (gate_crossed, up_crossed, *down_crossed),
        (gate_near, up_near, down_near),
        (gate_far, up_far, *down_far),
    )
    returned = lax.all_to_all(produced, ("chip", "dp"), split_axis=0, concat_axis=0, tiled=True)
    return combined(combine.reshape(rows, chips * depths * CAP), returned, hidden)


def solution(mesh):
    split = Mesh(mesh.devices.reshape(-1, 2, mesh.shape["dp"]), ALL)
    in_specs = (
        P(ALL, None),
        P(ALL, None),
        P(ALL, None),
        P(ALL, None),
        P(ALL, None, None),
        P(ALL, None, None),
        P(ALL),
        P(EP, None),
        P(),
        P(),
        P(ALL, None),
        P(ALL, None, None),
        P(ALL, None, None),
        P(ALL, None, None),
    )

    return jax.shard_map(
        local, mesh=split, in_specs=in_specs, out_specs=P(ALL, None), check_vma=False
    )
```

```python
import math

import jax
import jax.numpy as jnp
from jax import lax
from jax.experimental import pallas as pl
from jax.experimental.pallas import tpu as pltpu
from jax.sharding import Mesh
from jax.sharding import PartitionSpec as P

D = 4096
H = 64
KVH = 4
HD = 128
CAP = 4
ATTN_STEPS = 2
OUT_STEPS = 4
CUTS = 1
X_CUTS = 2
AHEAD = 2
COMBINE_STEPS = 2


EP = ("chip", "core")
ALL = ("chip", "core", "dp")


def flipped(value, axis, mask):
    pairs = [(source, source ^ mask) for source in range(lax.axis_size(axis))]
    return lax.ppermute(value, axis, pairs)


def attention_kernel(swap, lengths, q_in, nk_in, nv_in, keys, values, out, q_buf, o_buf):
    step = pl.program_id(0)
    tokens = q_in.shape[0]
    group = H // KVH
    scale = 1.0 / math.sqrt(HD)

    @pl.when(step == 0)
    def _():
        for head in range(H):
            q_buf[pl.ds(head, tokens, stride=H), :] = q_in[:, head * HD : (head + 1) * HD].astype(
                jnp.float32
            )

    nk = nk_in[...].astype(jnp.float32)
    nv = nv_in[...].astype(jnp.float32)
    span = keys.shape[1]
    owner = lax.broadcasted_iota(jnp.int32, (H, HD), 0) // group
    position = lax.broadcasted_iota(jnp.int32, (H, span), 1)
    each = keys.shape[0]
    base = step * each
    q_all = q_buf[pl.ds(base * H, each * H), :]

    def fanned(value):
        return jnp.concatenate(
            [
                jnp.broadcast_to(value[row : row + 1, g * HD : (g + 1) * HD], (group, HD))
                for row in range(each)
                for g in range(KVH)
            ],
            axis=0,
        )

    past = []
    for row in range(each):
        q = q_all[row * H : (row + 1) * H]
        blocks = [jnp.where(owner == g, q, 0.0).astype(jnp.bfloat16) for g in range(KVH)]
        scores = scale * lax.dot_general(
            jnp.concatenate(blocks, axis=1),
            keys[row],
            (((1,), (1,)), ((), ())),
            preferred_element_type=jnp.float32,
        )
        past.append(jnp.where(position < lengths[base + row], scores, -1e30))
    past = jnp.concatenate(past, axis=0)
    own = scale * jnp.sum(q_all * fanned(nk), axis=1, keepdims=True)
    peak = jnp.maximum(jnp.max(past, axis=1, keepdims=True), own)
    past_exp = jnp.exp(past - peak)
    own_exp = jnp.exp(own - peak)
    denom = jnp.sum(past_exp, axis=1, keepdims=True) + own_exp
    weights = (past_exp / denom).astype(jnp.bfloat16)
    own_part = (own_exp / denom).astype(jnp.bfloat16).astype(jnp.float32) * fanned(nv)
    for row in range(each):
        wide = jnp.dot(
            weights[row * H : (row + 1) * H], values[row], preferred_element_type=jnp.float32
        )
        blended = jnp.concatenate(
            [wide[g * group : (g + 1) * group, g * HD : (g + 1) * HD] for g in range(KVH)], axis=0
        )
        o_buf[pl.ds((base + row) * H, H), :] = blended + own_part[row * H : (row + 1) * H]

    @pl.when(step == pl.num_programs(0) - 1)
    def _():
        chips, _, width = out.shape
        per = width // HD
        for chip in range(chips):
            for at in range(per):
                head = chip * per + at
                first = o_buf[pl.ds(head, tokens, stride=H), :]
                second = o_buf[pl.ds(chip * per + (at ^ (per // 2)), tokens, stride=H), :]
                out[chip, :, at * HD : (at + 1) * HD] = jnp.where(
                    swap[0] == 1, second, first
                ).astype(jnp.bfloat16)


def attention(swap, queries, new_keys, new_values, cache_keys, cache_values, cache_len, chips):
    rows = queries.shape[0]
    span = cache_keys.shape[1]
    each = rows // ATTN_STEPS
    smem = pl.BlockSpec(memory_space=pltpu.SMEM)
    return pl.pallas_call(
        attention_kernel,
        grid=(ATTN_STEPS,),
        out_shape=jax.ShapeDtypeStruct((chips, rows, H * HD // chips), jnp.bfloat16),
        in_specs=[
            smem,
            smem,
            pl.BlockSpec((rows, H * HD), lambda i: (0, 0)),
            pl.BlockSpec((each, KVH * HD), lambda i: (i, 0)),
            pl.BlockSpec((each, KVH * HD), lambda i: (i, 0)),
            pl.BlockSpec((each, span, KVH * HD), lambda i: (i, 0, 0)),
            pl.BlockSpec((each, span, KVH * HD), lambda i: (i, 0, 0)),
        ],
        out_specs=pl.BlockSpec((chips, rows, H * HD // chips), lambda i: (0, 0, 0)),
        scratch_shapes=[
            pltpu.VMEM((rows * H, HD), jnp.float32),
            pltpu.VMEM((rows * H, HD), jnp.float32),
        ],
        compiler_params=pltpu.CompilerParams(dimension_semantics=("arbitrary",)),
        cost_estimate=pl.CostEstimate(
            flops=8 * rows * H * HD * span, bytes_accessed=4 * rows * span * KVH * HD, transcendentals=0
        ),
        name="attention",
    )(swap, cache_len, queries, new_keys, new_values, cache_keys, cache_values)


def ffn_kernel(flag, order, early, late, *refs):
    own, crossed, near, far = refs[0:3], refs[3:7], refs[7:10], refs[10:14]
    out, x_buf, in_buf, down_buf, y_buf, x_sem, in_sem, down_sem, y_sem = refs[14:]
    hf = own[0].shape[2]
    deep = D // CUTS
    wide = D // OUT_STEPS
    depths = order.shape[0]
    chips = out.shape[0] // depths

    def x_copy(cut):
        source = (early, late)[cut]
        deep_rows = source.shape[0]
        return pltpu.make_async_copy(
            source, x_buf.at[pl.ds(cut * deep_rows, deep_rows)], x_sem.at[cut]
        )

    def in_copy(side, source, part, cut):
        return pltpu.make_async_copy(
            source[part].at[0, pl.ds(cut * deep, deep)],
            in_buf.at[2 * side + part, pl.ds(cut * deep, deep)],
            in_sem.at[2 * side + part, cut],
        )

    def down_copy(row, source, step):
        return pltpu.make_async_copy(
            source.at[0, :, pl.ds(step * wide, wide)],
            down_buf.at[pl.ds(row, source.shape[1]), pl.ds(step * wide, wide)],
            down_sem.at[(4 * row) // hf, step],
        )

    def down_copies(first, second, step):
        return (
            down_copy(0, first[2], step),
            down_copy(hf, second[2], step),
            down_copy(hf + second[2].shape[1], second[3], step),
        )

    def slab(first, second, at):
        for cut in range(CUTS):
            in_copy(at // 2, (first, second)[at // 2], at % 2, cut).start()

    def downs(first, second, at):
        for step in range(OUT_STEPS):
            for copy in down_copies(first, second, step):
                copy.start()

    def start(task, at):
        @pl.when(flag[0] == 1)
        def _():
            task(own, crossed, at)

        @pl.when(flag[0] != 1)
        def _():
            task(near, far, at)

    for cut in range(X_CUTS):
        x_copy(cut).start()
    for at in range(AHEAD):
        start(slab, at)
    for cut in range(X_CUTS):
        x_copy(cut).wait()
    acts = []
    for side in range(2):
        vals = []
        for part in range(2):
            at = 2 * side + part
            for cut in range(CUTS):
                in_copy(side, own, part, cut).wait()
            if at + AHEAD < 4:
                start(slab, at + AHEAD)
            elif at + AHEAD == 4:
                start(downs, 0)
            vals.append(jnp.dot(x_buf[...], in_buf[at], preferred_element_type=jnp.float32))
        gate_val, up_val = vals
        acts.append((gate_val / (1.0 + jnp.exp(-gate_val)) * up_val).astype(jnp.bfloat16))
    act = jnp.concatenate(acts, axis=1)
    copies = []
    for step in range(OUT_STEPS):
        columns = slice(step * wide, (step + 1) * wide)
        for copy in down_copies(own, crossed, step):
            copy.wait()
        rows_out = jnp.dot(act, down_buf[:, columns], preferred_element_type=jnp.float32)
        for chunk in range(out.shape[0]):
            part, chip, turn = chunk // (2 * chips), chunk // 2 % chips, chunk % 2
            y_buf[chip * depths + order[2 * part + turn], :, columns] = rows_out[
                chunk * CAP : (chunk + 1) * CAP
            ].astype(jnp.bfloat16)
        copy = pltpu.make_async_copy(
            y_buf.at[:, :, pl.ds(step * wide, wide)],
            out.at[:, :, pl.ds(step * wide, wide)],
            y_sem.at[step],
        )
        copy.start()
        copies.append(copy)
    for copy in copies:
        copy.wait()


def expert_ffn(flag, order, early, late, own, crossed, near, far):
    count = early.shape[0] + late.shape[0]
    hf = own[0].shape[2]
    return pl.pallas_call(
        ffn_kernel,
        out_shape=jax.ShapeDtypeStruct((count // CAP, CAP, D), jnp.bfloat16),
        in_specs=[pl.BlockSpec(memory_space=pltpu.SMEM)] * 2
        + [pl.BlockSpec(memory_space=pltpu.HBM)] * 16,
        out_specs=pl.BlockSpec(memory_space=pltpu.HBM),
        scratch_shapes=[
            pltpu.VMEM((count, D), jnp.bfloat16),
            pltpu.VMEM((4, D, hf), jnp.bfloat16),
            pltpu.VMEM((2 * hf, D), jnp.bfloat16),
            pltpu.VMEM((count // CAP, CAP, D), jnp.bfloat16),
            pltpu.SemaphoreType.DMA((X_CUTS,)),
            pltpu.SemaphoreType.DMA((4, CUTS)),
            pltpu.SemaphoreType.DMA((8, OUT_STEPS)),
            pltpu.SemaphoreType.DMA((OUT_STEPS,)),
        ],
        compiler_params=pltpu.CompilerParams(vmem_limit_bytes=123 * 512 * 1024),
        cost_estimate=pl.CostEstimate(
            flops=12 * count * D * hf, bytes_accessed=12 * D * hf + 4 * count * D, transcendentals=0
        ),
        name="expert_ffn",
    )(flag, order, early, late, *own, *crossed, *near, *far)


def combine_kernel(weights, rows_in, hidden, out):
    flat = jnp.concatenate([rows_in[chunk] for chunk in range(rows_in.shape[0])], axis=0)
    out[...] = hidden[...] + jnp.dot(weights[...], flat, preferred_element_type=jnp.float32)


def combined(weights, rows_in, hidden):
    chunks, each, _ = rows_in.shape
    rows = hidden.shape[0]
    wide = D // COMBINE_STEPS
    return pl.pallas_call(
        combine_kernel,
        grid=(COMBINE_STEPS,),
        out_shape=jax.ShapeDtypeStruct((rows, D), jnp.float32),
        in_specs=[
            pl.BlockSpec((rows, chunks * each), lambda i: (0, 0)),
            pl.BlockSpec((chunks, each, wide), lambda i: (0, 0, i)),
            pl.BlockSpec((rows, wide), lambda i: (0, i)),
        ],
        out_specs=pl.BlockSpec((rows, wide), lambda i: (0, i)),
        compiler_params=pltpu.CompilerParams(
            dimension_semantics=("arbitrary",), vmem_limit_bytes=123 * 512 * 1024
        ),
        cost_estimate=pl.CostEstimate(
            flops=2 * rows * chunks * each * D, bytes_accessed=2 * chunks * each * D, transcendentals=0
        ),
        name="combined",
    )(weights, rows_in, hidden)


def local(
    resid,
    queries,
    new_keys,
    new_values,
    cache_keys,
    cache_values,
    cache_len,
    out_proj,
    norm_gain,
    router,
    expert_ids,
    gate_slab,
    up_slab,
    down_slab,
):
    rows = resid.shape[0]
    chips = lax.axis_size("chip")
    core = lax.axis_index("core")
    depth = lax.axis_index("dp")
    depths = lax.axis_size("dp")

    other_proj = flipped(out_proj, "core", 1)
    spots = [(c, d) for c in range(2) for d in range(depths)]
    across = [(c * depths + d, c * depths + (d ^ 1)) for c, d in spots if c != d % 2]
    beside = [(c * depths + d, (1 - c) * depths + d) for c, d in spots if c == d % 2]

    def moved(slab, pairs, after=None):
        if after is not None:
            slab, _ = lax.optimization_barrier((slab, after))
        return lax.ppermute(slab, ("core", "dp"), pairs)

    gate_crossed = moved(gate_slab, across)
    gate_near = moved(gate_slab, beside)
    up_near = moved(up_slab, beside)
    down_near = moved(down_slab, beside)
    flag = (core == depth % 2).astype(jnp.int32).reshape(1)
    ring = [(c * depths + d, c * depths + (d + 1 - 2 * c) % depths) for c, d in spots]

    def gathered(value):
        blocks = [value]
        for _ in range(depths - 1):
            blocks.append(lax.ppermute(blocks[-1], ("core", "dp"), ring))
        return blocks

    id_blocks = gathered(expert_ids)
    ids = jnp.concatenate(id_blocks, axis=0)

    piece = out_proj.shape[0]
    sent = attention(
        core.astype(jnp.int32).reshape(1),
        queries,
        new_keys,
        new_values,
        cache_keys,
        cache_values,
        cache_len,
        chips,
    )
    regrouped = lax.all_to_all(sent, "chip", split_axis=0, concat_axis=0, tiled=True)
    regrouped = regrouped.reshape(chips * rows, 2 * piece)
    partial = jnp.dot(regrouped[:, :piece], out_proj, preferred_element_type=jnp.float32)
    partial = partial + jnp.dot(
        regrouped[:, piece:], other_proj, preferred_element_type=jnp.float32
    )
    count = ids.shape[0]
    labels = 4 * jnp.arange(chips, dtype=jnp.int32) + 2 * (depth % 2) + depth // 2
    hits = ids.T[:, None, :] == labels[None, :, None]
    member = jnp.any(hits, axis=0)
    at = jnp.arange(count, dtype=jnp.int32)
    before = (at[:, None] < at[None, :]) & (at[:, None] // rows == at[None, :] // rows)
    rank = jnp.dot(
        member.astype(jnp.bfloat16),
        before.astype(jnp.bfloat16),
        preferred_element_type=jnp.float32,
    ).astype(jnp.int32)
    place = jnp.where(member, rank + CAP * (at // rows % 2)[None, :], -1)
    slots = CAP * 2
    dispatch = place[:, None, :] == jnp.arange(slots, dtype=jnp.int32)[None, :, None]

    chunk = jnp.arange(chips * depths, dtype=jnp.int32)
    homes = 4 * (chunk // depths) + 2 * (chunk % 2) + (chunk % depths) // 2
    own_hits = expert_ids[:, :, None] == homes[None, None, :]
    own_member = jnp.any(own_hits, axis=1)
    turn = jnp.arange(rows, dtype=jnp.int32)
    own_rank = jnp.dot(
        (turn[None, :] < turn[:, None]).astype(jnp.bfloat16),
        own_member.astype(jnp.bfloat16),
        preferred_element_type=jnp.float32,
    ).astype(jnp.int32)
    own_rank = jnp.where(own_member, own_rank, -1)
    own_slots = own_rank[:, :, None] == jnp.arange(CAP, dtype=jnp.int32)[None, None, :]

    partial = partial.astype(jnp.bfloat16)
    gate_far = moved(gate_crossed, beside, partial)
    up_crossed = moved(up_slab, across, partial)
    middle = down_slab.shape[1] // 8 * 7
    held, _ = lax.optimization_barrier((down_slab, partial))
    halves = lax.optimization_barrier((held[:, :middle], held[:, middle:]))
    most = moved(halves[0], across)
    rest = moved(halves[1], across)
    down_crossed = (most, rest)
    partial = lax.all_to_all(
        partial.reshape(chips, rows, D), "chip", split_axis=0, concat_axis=0, tiled=True
    )
    partial, dispatch, own_slots = lax.optimization_barrier((partial, dispatch, own_slots))
    hidden = resid.astype(jnp.float32) + jnp.sum(partial.astype(jnp.float32), axis=0)
    meansq = jnp.mean(hidden * hidden, axis=1, keepdims=True)
    normed = (hidden * lax.rsqrt(jnp.maximum(meansq, 0.25)) * norm_gain).astype(jnp.bfloat16)

    blocks = gathered(normed)
    half = count // 2
    outgoing = [
        jnp.dot(
            dispatch[:, :, part * half : (part + 1) * half]
            .reshape(chips * slots, half)
            .astype(jnp.bfloat16),
            jnp.concatenate(blocks[2 * part : 2 * part + 2], axis=0),
            preferred_element_type=jnp.float32,
        ).astype(jnp.bfloat16)
        for part in range(2)
    ]
    up_far = moved(up_crossed, beside, outgoing[1])
    down_far = [moved(half, beside, outgoing[1]) for half in down_crossed]
    incoming = []
    for part in range(2):
        incoming.append(
            lax.all_to_all(
                outgoing[part].reshape(chips, slots, D),
                "chip",
                split_axis=0,
                concat_axis=0,
                tiled=True,
            ).reshape(chips * slots, D)
        )

    logits = jnp.dot(normed, router, preferred_element_type=jnp.float32)
    experts = router.shape[1]
    onehot = expert_ids[:, :, None] == jnp.arange(experts, dtype=jnp.int32)[None, None, :]
    chosen = jnp.sum(jnp.where(onehot, logits[:, None, :], 0.0), axis=2)
    peak_logit = jnp.max(chosen, axis=1, keepdims=True)
    exp_logit = jnp.exp(chosen - peak_logit)
    gate_probs = (exp_logit / jnp.sum(exp_logit, axis=1, keepdims=True)).astype(jnp.bfloat16)
    spread = jnp.sum(jnp.where(own_hits, gate_probs.astype(jnp.float32)[:, :, None], 0.0), axis=1)
    combine = jnp.where(own_slots, spread[:, :, None], 0.0).astype(jnp.bfloat16)

    produced = expert_ffn(
        flag,
        (depth + depths + (2 * core - 1) * jnp.arange(depths, dtype=jnp.int32)) % depths,
        incoming[0],
        incoming[1],
        (gate_slab, up_slab, down_slab),
        (gate_crossed, up_crossed, *down_crossed),
        (gate_near, up_near, down_near),
        (gate_far, up_far, *down_far),
    )
    returned = lax.all_to_all(produced, ("chip", "dp"), split_axis=0, concat_axis=0, tiled=True)
    return combined(combine.reshape(rows, chips * depths * CAP), returned, hidden)


def solution(mesh):
    split = Mesh(mesh.devices.reshape(-1, 2, mesh.shape["dp"]), ALL)
    in_specs = (
        P(ALL, None),
        P(ALL, None),
        P(ALL, None),
        P(ALL, None),
        P(ALL, None, None),
        P(ALL, None, None),
        P(ALL),
        P(EP, None),
        P(),
        P(),
        P(ALL, None),
        P(ALL, None, None),
        P(ALL, None, None),
        P(ALL, None, None),
    )

    return jax.shard_map(
        local, mesh=split, in_specs=in_specs, out_specs=P(ALL, None), check_vma=False
    )
```
